8 devices in a mesh: layer: 1 (over z), tp: 2 (over y), fsdp: 4 (over x, core).
Axes of the slice: x: 2, y: 2, z: 1, core: 2. Of those that a mesh axis runs over, the one named last changes fastest.
Arguments:
- wq_weight: float32 [1024, 1024], P(('layer', 'fsdp'), 'tp')
- wq_moment: float32 [1024, 1024], P(('layer', 'fsdp'), 'tp')
- wq_grad: bfloat16 [1024, 1024], P(('layer', 'fsdp'), 'tp')
- wq_factor: float32 [1024, 64], P(('layer', 'tp'))
- wk_weight: float32 [1024, 512], P(('layer', 'fsdp'), 'tp')
- wk_moment: float32 [1024, 512], P(('layer', 'fsdp'), 'tp')
- wk_grad: bfloat16 [1024, 512], P(('layer', 'fsdp'), 'tp')
- wk_factor: float32 [512, 32], P(('layer', 'tp'))
- wv_weight: float32 [1024, 512], P(('layer', 'fsdp'), 'tp')
- wv_moment: float32 [1024, 512], P(('layer', 'fsdp'), 'tp')
- wv_grad: bfloat16 [1024, 512], P(('layer', 'fsdp'), 'tp')
- wv_factor: float32 [512, 32], P(('layer', 'tp'))
- wo_weight: float32 [1024, 1024], P(('layer', 'fsdp'), 'tp')
- wo_moment: float32 [1024, 1024], P(('layer', 'fsdp'), 'tp')
- wo_grad: bfloat16 [1024, 1024], P(('layer', 'fsdp'), 'tp')
- wo_factor: float32 [1024, 64], P(('layer', 'tp'))
- gate_weight: float32 [32, 1024, 512], P('layer', 'fsdp', 'tp')
- gate_moment: float32 [32, 1024, 512], P('layer', 'fsdp', 'tp')
- gate_grad: bfloat16 [32, 1024, 512], P('layer', 'fsdp', 'tp')
- gate_factor: float32 [32, 512, 32], P('layer', 'tp')
- up_weight: float32 [32, 1024, 512], P('layer', 'fsdp', 'tp')
- up_moment: float32 [32, 1024, 512], P('layer', 'fsdp', 'tp')
- up_grad: bfloat16 [32, 1024, 512], P('layer', 'fsdp', 'tp')
- up_factor: float32 [32, 512, 32], P('layer', 'tp')
- down_weight: float32 [32, 512, 1024], P('layer', 'fsdp', 'tp')
- down_moment: float32 [32, 512, 1024], P('layer', 'fsdp', 'tp')
- down_grad: bfloat16 [32, 512, 1024], P('layer', 'fsdp', 'tp')
- down_factor: float32 [32, 512, 32], P('layer', 'fsdp')
Outputs:
- output 1: float32 [1024, 1024], P(('layer', 'fsdp'), 'tp')
- output 2: float32 [1024, 1024], P(('layer', 'fsdp'), 'tp')
- output 3: float32 [1024, 64], P(('layer', 'tp'))
- output 4: float32 [1024, 512], P(('layer', 'fsdp'), 'tp')
- output 5: float32 [1024, 512], P(('layer', 'fsdp'), 'tp')
- output 6: float32 [512, 32], P(('layer', 'tp'))
- output 7: float32 [1024, 512], P(('layer', 'fsdp'), 'tp')
- output 8: float32 [1024, 512], P(('layer', 'fsdp'), 'tp')
- output 9: float32 [512, 32], P(('layer', 'tp'))
- output 10: float32 [1024, 1024], P(('layer', 'fsdp'), 'tp')
- output 11: float32 [1024, 1024], P(('layer', 'fsdp'), 'tp')
- output 12: float32 [1024, 64], P(('layer', 'tp'))
- output 13: float32 [32, 1024, 512], P('layer', 'fsdp', 'tp')
- output 14: float32 [32, 1024, 512], P('layer', 'fsdp', 'tp')
- output 15: float32 [32, 512, 32], P('layer', 'tp')
- output 16: float32 [32, 1024, 512], P('layer', 'fsdp', 'tp')
- output 17: float32 [32, 1024, 512], P('layer', 'fsdp', 'tp')
- output 18: float32 [32, 512, 32], P('layer', 'tp')
- output 19: float32 [32, 512, 1024], P('layer', 'fsdp', 'tp')
- output 20: float32 [32, 512, 1024], P('layer', 'fsdp', 'tp')
- output 21: float32 [32, 512, 32], P('layer', 'fsdp')
All inputs are finite; a program needn't handle non-finite values.
Results may differ from the reference program's by a relative error of at most 0.001.
Values are sent between devices in bfloat16 or wider.
A program may use at most 1 GiB of HBM per device.

```python
import math
import jax
import jax.numpy as jnp
from jax import lax

D = 1024
HEADS = 16
KV_HEADS = 8
HEAD = 64
FF = 512
EXPERTS = 32
RANK_DIV = 16

MOMENTUM = 0.9
LEARN_RATE = 0.3
FULL_PREC = lax.Precision.HIGHEST


def draw_matrix(rand_key, n_rows, n_cols, n_side):
    sub_keys = jax.random.split(rand_key, 9)
    row_grad = jax.random.uniform(sub_keys[0], (n_rows, 1), jnp.float32, 0.5, 1.5)
    col_grad = jax.random.uniform(sub_keys[1], (1, n_cols), jnp.float32, 0.5, 1.5)
    row_mom = jax.random.uniform(sub_keys[2], (n_rows, 1), jnp.float32, 0.5, 1.5)
    col_mom = jax.random.uniform(sub_keys[3], (1, n_cols), jnp.float32, 0.5, 1.5)
    weight = jax.random.normal(sub_keys[4], (n_rows, n_cols), jnp.float32) * n_rows ** -0.5
    moment = 0.5 * jax.random.normal(sub_keys[5], (n_rows, n_cols), jnp.float32) * row_mom * col_mom
    gradient = (jax.random.normal(sub_keys[6], (n_rows, n_cols), jnp.float32) * row_grad * col_grad).astype(jnp.bfloat16)
    rank_cols = n_side // RANK_DIV
    col_fac = jax.random.uniform(sub_keys[7], (1, rank_cols), jnp.float32, 0.7, 1.3)
    factor = jax.random.normal(sub_keys[8], (n_side, rank_cols), jnp.float32) * col_fac * n_side ** -0.5
    return weight, moment, gradient, factor


def setup_inputs(seed: int = 0, part: int = 0) -> dict:
    part_key = jax.random.fold_in(jax.random.key(seed), part)
    mat_keys = jax.random.split(part_key, 7)
    q_width = HEADS * HEAD
    kv_width = KV_HEADS * HEAD
    drawn = [
        ('wq', draw_matrix(mat_keys[0], D, q_width, q_width)),
        ('wk', draw_matrix(mat_keys[1], D, kv_width, kv_width)),
        ('wv', draw_matrix(mat_keys[2], D, kv_width, kv_width)),
        ('wo', draw_matrix(mat_keys[3], q_width, D, D)),
        ('gate', jax.vmap(lambda sub_key: draw_matrix(sub_key, D, FF, FF))(jax.random.split(mat_keys[4], EXPERTS))),
        ('up', jax.vmap(lambda sub_key: draw_matrix(sub_key, D, FF, FF))(jax.random.split(mat_keys[5], EXPERTS))),
        ('down', jax.vmap(lambda sub_key: draw_matrix(sub_key, FF, D, FF))(jax.random.split(mat_keys[6], EXPERTS))),
    ]
    inputs = {}
    for prefix, arrays in drawn:
        for suffix, drawn_arr in zip(('weight', 'moment', 'grad', 'factor'), arrays):
            inputs[prefix + '_' + suffix] = drawn_arr
    return inputs


def dion_one(weight, moment, gradient, factor):
    mom_grad = moment + gradient.astype(jnp.float32)
    p_tilde = jnp.dot(mom_grad, factor, preferred_element_type=jnp.float32, precision=FULL_PREC)
    gram_mat = jnp.dot(p_tilde.T, p_tilde, preferred_element_type=jnp.float32, precision=FULL_PREC)
    chol_low = jnp.linalg.cholesky(gram_mat)
    p_orth = lax.linalg.triangular_solve(chol_low, p_tilde, left_side=False, lower=True, transpose_a=True)
    r_new = jnp.dot(mom_grad.T, p_orth, preferred_element_type=jnp.float32, precision=FULL_PREC)
    moment_new = mom_grad - (1.0 - MOMENTUM) * jnp.dot(p_orth, r_new.T, preferred_element_type=jnp.float32, precision=FULL_PREC)
    col_norm = jnp.sqrt(jnp.sum(r_new * r_new, axis=0, keepdims=True))
    factor_new = r_new / col_norm
    step_scale = LEARN_RATE * math.sqrt(mom_grad.shape[0] / mom_grad.shape[1])
    weight_new = weight - step_scale * jnp.dot(p_orth, factor_new.T, preferred_element_type=jnp.float32, precision=FULL_PREC)
    return weight_new, moment_new, factor_new


def dion_flip(weight, moment, gradient, factor):
    weight_new, moment_new, factor_new = dion_one(weight.T, moment.T, gradient.T, factor)
    return weight_new.T, moment_new.T, factor_new


def reference(wq_weight, wq_moment, wq_grad, wq_factor, wk_weight, wk_moment, wk_grad, wk_factor, wv_weight, wv_moment, wv_grad, wv_factor, wo_weight, wo_moment, wo_grad, wo_factor, gate_weight, gate_moment, gate_grad, gate_factor, up_weight, up_moment, up_grad, up_factor, down_weight, down_moment, down_grad, down_factor):
    wq_new = dion_one(wq_weight, wq_moment, wq_grad, wq_factor)
    wk_new = dion_one(wk_weight, wk_moment, wk_grad, wk_factor)
    wv_new = dion_one(wv_weight, wv_moment, wv_grad, wv_factor)
    wo_new = dion_one(wo_weight, wo_moment, wo_grad, wo_factor)
    gate_new = lax.map(lambda per_expert: dion_one(per_expert[0], per_expert[1], per_expert[2], per_expert[3]), (gate_weight, gate_moment, gate_grad, gate_factor))
    up_new = lax.map(lambda per_expert: dion_one(per_expert[0], per_expert[1], per_expert[2], per_expert[3]), (up_weight, up_moment, up_grad, up_factor))
    down_new = lax.map(lambda per_expert: dion_flip(per_expert[0], per_expert[1], per_expert[2], per_expert[3]), (down_weight, down_moment, down_grad, down_factor))
    return (wq_new[0], wq_new[1], wq_new[2], wk_new[0], wk_new[1], wk_new[2], wv_new[0], wv_new[1], wv_new[2], wo_new[0], wo_new[1], wo_new[2], gate_new[0], gate_new[1], gate_new[2], up_new[0], up_new[1], up_new[2], down_new[0], down_new[1], down_new[2])
```

```python
import math
import jax
import jax.numpy as jnp
from jax import lax
from jax.experimental import pallas as pl
from jax.experimental.pallas import tpu as pltpu
from jax.sharding import PartitionSpec as P


MOMENTUM = 0.9
LEARN_RATE = 0.3
F32 = jnp.float32
BF = jnp.bfloat16
MESH = pl.DeviceIdType.MESH
NG = 8
PACK = 4
L = 128
H = 256
W = 512
R = 32
RD = 64
COMM_VMEM = 30 << 20
FINAL_VMEM = 30 << 20
SH = 72


def dot(a, b):
    return jnp.dot(a, b, preferred_element_type=F32)


def split3(x):
    a = x.astype(BF)
    r = x - a.astype(F32)
    b = r.astype(BF)
    c = (r - b.astype(F32)).astype(BF)
    return a, b, c


def iota(shape, axis):
    return lax.broadcasted_iota(jnp.int32, shape, axis)


def row_factor(pieces, count, v, rank):
    v1, v2, v3 = split3(v)
    group = iota((1, L), 1) // rank
    acc = acc2 = None
    for m in range(count):
        b12, b1, b3 = pieces(m)
        mask = jnp.where(group == m, 1.0, 0.0).astype(BF)
        w1, w2, w3 = v1 * mask, v2 * mask, v3 * mask
        t = dot(b12, jnp.concatenate([w1, w2], 1))
        u = dot(b1, w3) + dot(b3, w1)
        acc = t if acc is None else acc + t
        acc2 = u if acc2 is None else acc2 + u
    n = acc2.shape[0]
    return acc[:n, :L] + acc2 + (acc[:n, L:] + acc[n:, :L]) + acc[n:, L:]


def col_factor(ut, b1, b2, b3, m, rank):
    lhs = jnp.concatenate([t[rank * m:rank * m + rank] for t in ut], 0)
    o1 = dot(lhs, b1)
    o2 = dot(lhs[:2 * rank], b2)
    o3 = dot(lhs[:rank], b3)
    return o1[:rank] + (o1[rank:2 * rank] + o2[:rank]) + (o1[2 * rank:] + o2[rank:] + o3)


def gram(ut, u, rank):
    full = dot(jnp.concatenate([ut[0], ut[1]], 0), jnp.concatenate([u[0], u[1]], 1))
    low = dot(ut[2], u[0]) + dot(ut[0], u[2])
    g = full[:L, :L] + (full[:L, L:] + full[L:, :L] + low) + full[L:, L:]
    group = iota((rank, L), 1) // rank
    out = jnp.where(group == 0, g[:rank], 0.0)
    for m in range(1, L // rank):
        out = out + jnp.where(group == m, g[rank * m:rank * m + rank], 0.0)
    return out


def inverse_factors(grams, rank):
    lane = iota((rank, L), 1)
    row = iota((rank, L), 0)
    base = (lane // rank) * rank
    col = lane - base
    mats = list(grams)
    for k0 in range(0, rank, 8):
        cols = [[jnp.take_along_axis(a, base + (k0 + j), axis=1) for j in range(8)] for a in mats]
        for j in range(8):
            k = k0 + j
            below = row > k
            for i, a in enumerate(mats):
                ck = cols[i][j]
                factor = jnp.where(below, ck * (1.0 / ck[k:k + 1]), 0.0)
                pivot = jnp.where(col[:1] == k, 1.0, a[k:k + 1])
                mats[i] = jnp.where(below & (col == k), 0.0, a) - factor * pivot
                for l in range(j + 1, 8):
                    cl = cols[i][l]
                    cols[i][l] = cl - factor * cl[k:k + 1]
    out = []
    for a in mats:
        diag = jnp.take_along_axis(a, base + row, axis=1)
        unit = jnp.where(col < row, a, jnp.where(col == row, 1.0, 0.0))
        out.append(unit * (1.0 / jnp.sqrt(diag)))
    return out


def block_diag(inv, rank):
    group = iota((rank, L), 1) // rank
    return jnp.concatenate([jnp.where(group == m, inv, 0.0) for m in range(L // rank)], 0)


def times_right(u, t):
    u1, u2, u3 = split3(u)
    t1, t2, t3 = split3(t)
    t12 = jnp.concatenate([t1, t2], 1)
    a = dot(jnp.concatenate([u1, u2], 1), jnp.concatenate([t12, t12], 0))
    b = dot(jnp.concatenate([u1, u3], 1), jnp.concatenate([t3, t1], 0))
    return a[:, :L] + (a[:, L:] + b)


def times_left(b, v):
    b1, b2, b3 = split3(b)
    v1, v2, v3 = split3(v)
    b12 = jnp.concatenate([b1, b2], 1)
    hi = dot(b12, jnp.concatenate([v1, v1], 0))
    lo = dot(b12, jnp.concatenate([v2, v2], 0))
    lo = lo + dot(jnp.concatenate([b1, b3], 1), jnp.concatenate([v3, v1], 0))
    return hi + lo


def sq_rows_to_lanes(v):
    s = v * v
    f = s[:, :L]
    for i in range(1, v.shape[1] // L):
        f = f + s[:, L * i:L * i + L]
    return jnp.broadcast_to(jnp.sum(f.T, 0, keepdims=True), (8, L))


def sq_lanes(u):
    return jnp.broadcast_to(jnp.sum(u * u, 0, keepdims=True), (8, L))


def gram_to_rows(w, half, rank):
    h = rank // 2
    return jnp.concatenate([w[half * h + 8 * i:half * h + 8 * i + 8] for i in range(h // 8)], 1)


def rows_to_gram(halves, rank):
    parts = []
    for x in halves:
        parts.extend([x[:, L * i:L * i + L] for i in range(rank // 16)])
    return jnp.concatenate(parts, 0)


def comm_kernel(gm, gg, gq, um, ug, uq, dm, dg, dq,
                wqm, wqg, wqf, wkm, wkg, wkf, wvm, wvg, wvf, wom, wog, wof,
                b_e, b_d, b_kv, b_qo, e_inv, e_p, e_rt, e_n, d_r, d_pt, d_n,
                kv_inv, kv_p, kv_rt, kv_n, qo_inv, qo_p, qo_rt, qo_n,
                gs_e, gs_d, qs_e, qs_d, gs_kv, qs_kv, gs_qo, qs_qo,
                z_e, z_d, z_kv, z_qo,
                pown, prcv, down, drc1, dxs, dxr, ptf, sown, src1, sxs, sxr, stf, zown, zrcv,
                nown, nrcv, dnown, dnrcv,
                kpo, kpr, kso, ksr, kxs, kxr, kst, kno, knr,
                qpo, qpr, qso, qsr, qxs, qxr, qst, qno, qnr,
                lsem, dsem, send, recv, sendk, recvk, sendn, recvn):
    tp = lax.axis_index("tp")
    fs = lax.axis_index("fsdp")
    core = lax.rem(fs, 2)
    ypeer = {"tp": 1 - tp}
    sib = {"fsdp": fs + 1 - 2 * core}
    xpeer = {"fsdp": lax.rem(fs + 2, 4)}

    def loads(g):
        s = lax.rem(g, 2)
        e = pl.ds(g * PACK, PACK)
        pairs = [(gm.at[e], b_e.at[0, e]), (gg.at[e], gs_e.at[s, 0]), (gq.at[e], qs_e.at[s, 0]),
                 (um.at[e], b_e.at[1, e]), (ug.at[e], gs_e.at[s, 1]), (uq.at[e], qs_e.at[s, 1])]
        return [pltpu.make_async_copy(a, b, lsem.at[s, i]) for i, (a, b) in enumerate(pairs)]

    def loads_down(g):
        s = lax.rem(g, 2)
        e = pl.ds(g * PACK, PACK)
        pairs = [(dm.at[e], b_d.at[e]), (dg.at[e], gs_d.at[s]), (dq.at[e], qs_d.at[s])]
        return [pltpu.make_async_copy(a, b, lsem.at[s, len(pairs) * 2 + i]) for i, (a, b) in enumerate(pairs)]

    dense_loads = [pltpu.make_async_copy(a, b, dsem.at[i]) for i, (a, b) in enumerate([
        (wkm, b_kv.at[0]), (wkg, gs_kv.at[0]), (wkf, qs_kv.at[0]),
        (wvm, b_kv.at[1]), (wvg, gs_kv.at[1]), (wvf, qs_kv.at[1]),
        (wqm, b_qo.at[0]), (wqg, gs_qo.at[0]), (wqf, qs_qo.at[0]),
        (wom, b_qo.at[1]), (wog, gs_qo.at[1]), (wof, qs_qo.at[1])])]
    for c in dense_loads:
        c.start()

    barrier = pltpu.get_barrier_semaphore()
    fours = [{"fsdp": lax.rem(fs + i, 4)} for i in (1, 2, 3)]
    for dev in [ypeer] + fours:
        pl.semaphore_signal(barrier, inc=1, device_id=dev, device_id_type=MESH)
    pl.semaphore_wait(barrier, 4)

    def remote(src, dst, ss, rs, dev):
        return pltpu.make_async_remote_copy(src_ref=src, dst_ref=dst, send_sem=ss, recv_sem=rs,
                                            device_id=dev, device_id_type=MESH)

    def c_p(g, q):
        return remote(pown.at[lax.rem(g, 2), q], prcv.at[g, q], send.at[q, g], recv.at[q, g], ypeer)

    def c_d1(g):
        return remote(down.at[lax.rem(g, 2), 1 - core], drc1.at[g], send.at[2, g], recv.at[2, g], sib)

    def c_d2(g):
        return remote(dxs.at[lax.rem(g, 2)], dxr.at[g], send.at[3, g], recv.at[3, g], xpeer)

    def c_d3(g):
        return remote(ptf.at[g, core], ptf.at[g, core], send.at[4, g], recv.at[4, g], sib)

    def c_s1(g):
        return remote(sown.at[lax.rem(g, 2), 1 - core], src1.at[g], send.at[5, g], recv.at[5, g], sib)

    def c_s2(g):
        return remote(sxs.at[lax.rem(g, 2)], sxr.at[g], send.at[6, g], recv.at[6, g], xpeer)

    def c_s3(g):
        return remote(stf.at[g, core], stf.at[g, core], send.at[7, g], recv.at[7, g], sib)

    def c_z(g):
        return remote(zown.at[lax.rem(g, 2)], zrcv.at[g], send.at[8, g], recv.at[8, g], ypeer)

    def c_n(g):
        return remote(nown.at[g], nrcv.at[g], send.at[9, g], recv.at[9, g], ypeer)

    def c_nd(g):
        return [remote(dnown.at[g], dnrcv.at[g, i], sendn.at[i, g], recvn.at[i, g], fours[i]) for i in range(3)]

    def dense_copies(i, po, pr, so, sr, xs, xr, st, no, nr):
        k = lambda j: (sendk.at[i, j], recvk.at[i, j])
        return (lambda: remote(po, pr, *k(0), ypeer),
                lambda: remote(so.at[1 - core], sr, *k(1), sib),
                lambda: remote(xs, xr, *k(2), xpeer),
                lambda: remote(st.at[core], st.at[core], *k(3), sib),
                lambda: remote(no, nr, *k(4), ypeer))

    kc = dense_copies(0, kpo, kpr, kso, ksr, kxs, kxr, kst, kno, knr)
    qc = dense_copies(1, qpo, qpr, qso, qsr, qxs, qxr, qst, qno, qnr)

    def terms(b_ref, g_ref, z_ref):
        for r0 in range(0, b_ref.shape[0], RD):
            rs = pl.ds(r0, RD)
            b = b_ref[rs]
            if g_ref is not None:
                b = b + g_ref[rs].astype(F32)
                b_ref[rs] = b
            b1, b2, b3 = split3(b)
            z_ref[0, rs] = b1
            z_ref[1, rs] = b2
            z_ref[2, rs] = b3

    def pieces_of(z_ref):
        n, w = z_ref.shape[1:]
        return z_ref[0:2].reshape(2 * n, w), z_ref[0], z_ref[2]

    def stage1(g):
        s = lax.rem(g, 2)
        for c in loads(g):
            c.wait()

        def one(q, _):
            for m in range(PACK):
                terms(b_e.at[q, g * PACK + m], gs_e.at[s, q, m], z_e.at[m])
            v = qs_e[s, q].reshape(L, H).T
            pown[s, q] = row_factor(lambda m: pieces_of(z_e.at[m]), PACK, v, R)
            c_p(g, q).start()
            return 0

        lax.fori_loop(0, 2, one, 0)

    def stage1_down(g):
        s = lax.rem(g, 2)
        for c in loads_down(g):
            c.wait()
        ut = split3(qs_d[s].reshape(L, L))
        for m in range(PACK):
            terms(b_d.at[g * PACK + m], gs_d.at[s, m], z_d.at[m])
            part = col_factor(ut, z_d[m, 0], z_d[m, 1], z_d[m, 2], m, R)
            down[s, 0, pl.ds(R * m, R)] = part[:, :H]
            down[s, 1, pl.ds(R * m, R)] = part[:, H:]
        c_d1(g).start()

    def stage1_dense():
        for c in dense_loads:
            c.wait()
        for c in loads_down(0) + loads(0) + loads_down(1):
            c.start()
        for i in range(2):
            terms(b_kv.at[i], gs_kv.at[i], z_kv.at[i])
            terms(b_qo.at[i], gs_qo.at[i], z_qo.at[i])
        v = jnp.concatenate([qs_kv[0], qs_kv[1], qs_kv[0], qs_kv[1]], 0).T
        kpo[:] = row_factor(lambda m: pieces_of(z_kv.at[m % 2]), 4, v, R)
        kc[0]().start()
        v = qs_qo[:].reshape(L, W).T
        qpo[:] = row_factor(lambda m: pieces_of(z_qo.at[m]), 2, v, RD)
        qc[0]().start()

    def stage2a(g):
        s = lax.rem(g, 2)
        c_d1(g).wait()
        dxs[s] = down[s, core] + drc1[g]
        c_d2(g).start()

    def stage2b(g):
        c_d2(g).wait()
        ptf[g, core] = dxs[lax.rem(g, 2)] + dxr[g]
        c_d3(g).start()

    def s_and_gram(u, rank, count, z_of, so):
        ut = u.T
        up, utp = split3(u), split3(ut)
        half = L // rank // 2
        for m in range(count):
            z = z_of(m)
            so[m // half, pl.ds(rank * (m % half), rank)] = col_factor(utp, z[0], z[1], z[2], m, rank)
        w = gram(utp, up, rank)
        for h in range(2):
            so[h, pl.ds(RD, 8)] = gram_to_rows(w, h, rank)

    def stage2c(g):
        s = lax.rem(g, 2)

        def one(q, _):
            c_p(g, q).wait()
            u = pown[s, q] + prcv[g, q]
            e_p[g, q] = u
            for m in range(PACK):
                terms(b_e.at[q, g * PACK + m], None, z_e.at[m])
            s_and_gram(u, R, PACK, z_e.at.__getitem__, sown.at[s, :, q])
            return 0

        lax.fori_loop(0, 2, one, 0)
        c_s1(g).start()

    def stage2c_down(g):
        s = lax.rem(g, 2)
        for m in range(PACK):
            terms(b_d.at[g * PACK + m], None, z_d.at[m])
        c_d3(g).wait()
        vt = jnp.concatenate([ptf[g, 0], ptf[g, 1]], 1)
        d_pt[g] = vt
        v = vt.T
        zown[s, pl.ds(0, L)] = row_factor(lambda m: pieces_of(z_d.at[m]), PACK, v, R)
        zown[s, pl.ds(L, R)] = gram(split3(vt), split3(v), R)
        c_z(g).start()

    def stage2_dense():
        kc[0]().wait()
        u = kpo[:] + kpr[:]
        kv_p[:] = u
        s_and_gram(u, R, 4, lambda m: z_kv.at[m % 2], kso)
        kc[1]().start()
        qc[0]().wait()
        u = qpo[:] + qpr[:]
        qo_p[:] = u
        s_and_gram(u, RD, 2, lambda m: z_qo.at[m], qso)
        qc[1]().start()

    def stage3a(g):
        s = lax.rem(g, 2)
        c_s1(g).wait()
        sxs[s] = sown[s, core] + src1[g]
        c_s2(g).start()

    def stage3b(g):
        c_s2(g).wait()
        stf[g, core] = sxs[lax.rem(g, 2)] + sxr[g]
        c_s3(g).start()

    def stage3a_dense():
        for cs, so, sr, xs in ((kc, kso, ksr, kxs), (qc, qso, qsr, qxs)):
            cs[1]().wait()
            xs[:] = so[core] + sr[:]
            cs[2]().start()

    def stage3b_dense():
        for cs, xs, xr, st in ((kc, kxs, kxr, kst), (qc, qxs, qxr, qst)):
            cs[2]().wait()
            st[core] = xs[:] + xr[:]
            cs[3]().start()

    def apply_keep(rt_ref, n_ref, inv, st, rank):
        bd = block_diag(inv, rank)
        vt = jnp.concatenate([st[0, pl.ds(0, RD)], st[1, pl.ds(0, RD)]], 0)
        rt = times_left(bd, vt)
        rt_ref[:] = rt
        n_ref[:] = sq_rows_to_lanes(rt)

    def stage4(g):
        s = lax.rem(g, 2)
        c_s3(g).wait()
        c_z(g).wait()
        z = zown[s] + zrcv[g]
        ws = [rows_to_gram([stf[g, h, q, pl.ds(RD, 8)] for h in range(2)], R) for q in range(2)]
        inv = inverse_factors(ws + [z[L:]], R)
        for i in range(3):
            e_inv[g, i] = inv[i]
        for q in range(2):
            apply_keep(e_rt.at[g, q], nown.at[g, q], inv[q], stf.at[g, :, q], R)
        c_n(g).start()
        bd = block_diag(inv[2], R)
        r = times_right(z[:L], bd.T)
        d_r[g] = r
        dnown[g] = sq_lanes(r)
        for c in c_nd(g):
            c.start()

    def stage4_dense():
        kc[3]().wait()
        inv = inverse_factors([rows_to_gram([kst[h, pl.ds(RD, 8)] for h in range(2)], R)], R)
        kv_inv[:] = inv[0]
        apply_keep(kv_rt, kno, inv[0], kst, R)
        kc[4]().start()
        qc[3]().wait()
        inv = inverse_factors([rows_to_gram([qst[h, pl.ds(RD, 8)] for h in range(2)], RD)], RD)
        qo_inv[:] = inv[0]
        apply_keep(qo_rt, qno, inv[0], qst, RD)
        qc[4]().start()

    def stage5(g):
        c_n(g).wait()
        for q in range(2):
            e_n[g, q] = 1.0 / jnp.sqrt(nown[g, q] + nrcv[g, q])
        for c in c_nd(g):
            c.wait()
        d_n[g] = 1.0 / jnp.sqrt((dnown[g] + dnrcv[g, 1]) + (dnrcv[g, 0] + dnrcv[g, 2]))

    def stage5_dense():
        kc[4]().wait()
        kv_n[:] = 1.0 / jnp.sqrt(kno[:] + knr[:])
        qc[4]().wait()
        qo_n[:] = 1.0 / jnp.sqrt(qno[:] + qnr[:])

    stage1_dense()
    stage1_down(0)

    def step(t, _):
        def within(lag, stage):
            @pl.when((t >= lag) & (t < NG + lag))
            def _():
                stage(t - lag)

        def only(at, stage):
            @pl.when(t == at)
            def _():
                stage()

        @pl.when(t < NG - 1)
        def _():
            for c in loads(t + 1):
                c.start()

        @pl.when(t < NG - 2)
        def _():
            for c in loads_down(t + 2):
                c.start()

        within(0, stage2a)
        within(0, stage1)

        @pl.when(t < NG - 1)
        def _():
            stage1_down(t + 1)

        within(1, stage2b)
        within(3, stage5)
        only(2, stage5_dense)
        only(0, stage2_dense)
        within(1, stage2c)
        within(2, stage3b)
        only(1, stage3b_dense)
        within(1, stage2c_down)
        within(1, stage3a)
        only(0, stage3a_dense)
        within(2, stage4)
        only(1, stage4_dense)
        return 0

    lax.fori_loop(0, NG + 3, step, 0)


def run_comm(args):
    v = pltpu.VMEM
    dma = pltpu.SemaphoreType.DMA
    out = lambda *shape: v(shape, F32)
    out_shape = [out(2, R, H, H), out(R, L, W), out(2, H, H), out(2, H, W),
                 out(NG, 3, R, L), out(NG, 2, H, L), out(NG, 2, L, H), out(NG, 2, 8, L),
                 out(NG, L, L), out(NG, L, W), out(NG, 8, L),
                 out(R, L), out(H, L), out(L, H), out(8, L),
                 out(RD, L), out(H, L), out(L, W), out(8, L)]

    def pack_bufs(w):
        return [v((H, L), F32), v((H, L), F32), v((2, SH, w), F32), v((SH, w), F32), v((SH, w), F32),
                v((SH, w), F32), v((2, SH, w), F32), v((8, L), F32), v((8, L), F32)]

    scratch = [
        v((2, 2, 4, H, H), BF), v((2, 4, L, W), BF), v((2, 2, 4, R, H), F32), v((2, 4, R, L), F32),
        v((2, H, H), BF), v((2, R, H), F32), v((2, H, W), BF), v((2, RD, W), F32),
        v((4, 3, H, H), BF), v((4, 3, L, W), BF), v((2, 3, H, H), BF), v((2, 3, H, W), BF),
        v((2, 2, H, L), F32), v((NG, 2, H, L), F32),
        v((2, 2, L, H), F32), v((NG, L, H), F32), v((2, L, H), F32), v((NG, L, H), F32),
        v((NG, 2, L, H), F32),
        v((2, 2, 2, SH, H), F32), v((NG, 2, SH, H), F32), v((2, 2, SH, H), F32), v((NG, 2, SH, H), F32),
        v((NG, 2, 2, SH, H), F32),
        v((2, 160, L), F32), v((NG, 160, L), F32),
        v((NG, 2, 8, L), F32), v((NG, 2, 8, L), F32), v((NG, 8, L), F32), v((NG, 3, 8, L), F32),
    ] + pack_bufs(H) + pack_bufs(W) + [
        dma((2, 9)), dma((12,)), dma((10, NG)), dma((10, NG)), dma((2, 5)), dma((2, 5)), dma((3, NG)), dma((3, NG))]
    return pl.pallas_call(
        comm_kernel,
        out_shape=out_shape,
        in_specs=[pl.BlockSpec(memory_space=pl.ANY)] * 21,
        out_specs=[pl.BlockSpec(memory_space=pltpu.VMEM)] * len(out_shape),
        scratch_shapes=scratch,
        name="comm_kernel",
        compiler_params=pltpu.CompilerParams(collective_id=0, has_side_effects=True, vmem_limit_bytes=COMM_VMEM),
    )(*args)


def lane_copies(u, rank):
    count = L // rank
    group = iota((1, L), 1) // rank
    rolled = [u] + [pltpu.roll(u, rank * s, 1) for s in range(1, count)]
    outs = []
    for m in range(count):
        x = rolled[(0 - m) % count]
        for gidx in range(1, count):
            x = jnp.where(group == gidx, rolled[(gidx - m) % count], x)
        outs.append(x)
    return outs


def left_tiles(x, rank):
    a = x.astype(BF)
    r1 = x - a.astype(F32)
    b = r1.astype(BF)
    r2 = r1 - b.astype(F32)
    low = iota((1, L), 1) < RD
    if rank == R:
        return jnp.concatenate([a, jnp.where(low, r1, r2).astype(BF)], 1)
    return jnp.concatenate([a, jnp.where(low, x, r1).astype(BF), jnp.where(low, r1, r2).astype(BF)], 1)


def right_tiles(vt, rank):
    a, b, c = split3(vt)
    if rank == R:
        return jnp.concatenate([a, b, c, jnp.zeros_like(a), a, b, a, b], 0)
    return jnp.concatenate([a, b, c, a, b, a], 0)


def lanes_to_rows(n):
    return jnp.broadcast_to(n[:1], (L, L)).T


def scale_rows(vt, n):
    t = lanes_to_rows(n)
    return jnp.concatenate([vt[:, L * i:L * i + L] * t for i in range(vt.shape[1] // L)], 1)


def keep_update(p0, inv, rt, n, rank, slots, x_of, b_of, xo, mo, qo, step):
    copies = lane_copies(times_right(p0, block_diag(inv, rank).T), rank)
    rts = scale_rows(rt, n)
    for m in slots:
        lhs = left_tiles(copies[m], rank)
        rows = slice(rank * m, rank * m + rank)
        mo(m)[:] = b_of(m)[:] - dot(lhs, right_tiles(rt[rows] * (1.0 - MOMENTUM), rank))
        xo(m)[:] = x_of(m)[:] - dot(lhs, right_tiles(rts[rows] * step, rank))
        qo(m)[:] = rts[rows]


def final_kernel(gx, ux, dx, qx, kx, vx, ox,
                 b_e, b_d, b_kv, b_qo, e_inv, e_p, e_rt, e_n, d_r, d_pt, d_n,
                 kv_inv, kv_p, kv_rt, kv_n, qo_inv, qo_p, qo_rt, qo_n,
                 gxo, gmo, gqo, uxo, umo, uqo, dxo, dmo, dqo,
                 qxo, qmo, qqo, kxo, kmo, kqo, vxo, vmo, vqo, oxo, omo, oqo,
                 xs_kv, xs_qo, mt_kv, mt_qo, qt_kv, qt_qo, isem, osem):
    i = pl.program_id(0)
    step = LEARN_RATE * math.sqrt(2.0)
    ins = [pltpu.make_async_copy(a, b, isem.at[k]) for k, (a, b) in enumerate(
        [(kx, xs_kv.at[0]), (vx, xs_kv.at[1]), (qx, xs_qo.at[0]), (ox, xs_qo.at[1])])]
    outs = [pltpu.make_async_copy(b, a, osem.at[k]) for k, (a, b) in enumerate(
        [(kxo, xs_kv.at[0]), (vxo, xs_kv.at[1]), (qxo, xs_qo.at[0]), (oxo, xs_qo.at[1]),
         (kmo, mt_kv.at[0]), (vmo, mt_kv.at[1]), (qmo, mt_qo.at[0]), (omo, mt_qo.at[1]),
         (kqo, qt_kv.at[0]), (vqo, qt_kv.at[1]), (qqo, qt_qo.at[0]), (oqo, qt_qo.at[1])])]

    @pl.when(i == 0)
    def _():
        for c in ins:
            c.start()

    for q, (x, xo, mo, qo) in enumerate(((gx, gxo, gmo, gqo), (ux, uxo, umo, uqo))):
        keep_update(e_p[i, q], e_inv[i, q], e_rt[i, q], e_n[i, q], R, range(PACK),
                    x.at.__getitem__, lambda m: b_e.at[q, i * PACK + m],
                    xo.at.__getitem__, mo.at.__getitem__, qo.at.__getitem__, step)
    r = d_r[i]
    pt = times_left(block_diag(e_inv[i, 2], R), d_pt[i])
    qpack = r * d_n[i][:1]
    rcopies = lane_copies(r * (1.0 - MOMENTUM), R)
    qcopies = lane_copies(qpack * step, R)
    qrows = qpack.T
    for m in range(PACK):
        rhs = right_tiles(pt[R * m:R * m + R], R)
        dmo[m] = b_d[i * PACK + m] - dot(left_tiles(rcopies[m], R), rhs)
        dxo[m] = dx[m] - dot(left_tiles(qcopies[m], R), rhs)
        dqo[m] = qrows[R * m:R * m + R]

    @pl.when(i == 1)
    def _():
        for c in ins:
            c.wait()
        keep_update(kv_p[:], kv_inv[:], kv_rt[:], kv_n[:], R, range(2),
                    xs_kv.at.__getitem__, b_kv.at.__getitem__,
                    xs_kv.at.__getitem__, mt_kv.at.__getitem__, qt_kv.at.__getitem__, step)
        keep_update(qo_p[:], qo_inv[:], qo_rt[:], qo_n[:], RD, range(2),
                    xs_qo.at.__getitem__, b_qo.at.__getitem__,
                    xs_qo.at.__getitem__, mt_qo.at.__getitem__, qt_qo.at.__getitem__, LEARN_RATE)
        for c in outs:
            c.start()

    @pl.when(i == NG - 1)
    def _():
        for c in outs:
            c.wait()


def run_final(xs, packs):
    hbm = pl.BlockSpec(memory_space=pl.ANY)
    v = pltpu.VMEM

    def spec(a):
        return pl.BlockSpec((PACK,) + a.shape[1:], lambda i: (i, 0, 0))

    out = lambda *shape: jax.ShapeDtypeStruct(shape, F32)
    big = [out(R, H, H), out(R, H, H), out(R, R, H)]
    stacks = big + big + [out(R, L, W), out(R, L, W), out(R, R, L)]
    wide = [out(H, W), out(H, W), out(RD, W)]
    narrow = [out(H, H), out(H, H), out(R, H)]
    return pl.pallas_call(
        final_kernel,
        grid=(NG,),
        out_shape=stacks + wide + narrow + narrow + wide,
        in_specs=[spec(a) for a in xs[:3]] + [hbm] * 4 + [pl.BlockSpec(memory_space=v)] * len(packs),
        out_specs=[spec(a) for a in stacks] + [hbm] * 12,
        scratch_shapes=[v((2, H, H), F32), v((2, H, W), F32), v((2, H, H), F32), v((2, H, W), F32),
                        v((2, R, H), F32), v((2, RD, W), F32),
                        pltpu.SemaphoreType.DMA((4,)), pltpu.SemaphoreType.DMA((12,))],
        name="final_kernel",
        compiler_params=pltpu.CompilerParams(vmem_limit_bytes=FINAL_VMEM, dimension_semantics=("arbitrary",)),
    )(*xs, *packs)


def solution(mesh):
    dense_w = P(('layer', 'fsdp'), 'tp')
    dense_f = P(('layer', 'tp'), None)
    stack_w = P('layer', 'fsdp', 'tp')
    stack_f = P('layer', 'tp', None)
    down_f = P('layer', 'fsdp', None)
    in_specs = (dense_w, dense_w, dense_w, dense_f) * 4 + (stack_w, stack_w, stack_w, stack_f) * 2 + (stack_w, stack_w, stack_w, down_f)
    out_specs = (dense_w, dense_w, dense_f) * 4 + (stack_w, stack_w, stack_f) * 2 + (stack_w, stack_w, down_f)

    def local_step(*b):
        x, m, g = b[0::4], b[1::4], b[2::4]
        q = [jnp.swapaxes(f, -1, -2) for f in b[3::4]]
        comm_in = []
        for i in (4, 5, 6, 0, 1, 2, 3):
            comm_in += [m[i], g[i], q[i]]
        packs = [pltpu.with_memory_space_constraint(a, pltpu.VMEM) for a in run_comm(comm_in)]
        outs = run_final([x[i] for i in (4, 5, 6, 0, 1, 2, 3)], packs)
        outs = list(outs[9:]) + list(outs[:9])
        for i in range(2, 21, 3):
            outs[i] = jnp.swapaxes(outs[i], -1, -2)
        return tuple(outs)

    return jax.shard_map(local_step, mesh=mesh, in_specs=in_specs, out_specs=out_specs, check_vma=False)
```

```python
import math
import jax
import jax.numpy as jnp
from jax import lax
from jax.experimental import pallas as pl
from jax.experimental.pallas import tpu as pltpu
from jax.sharding import PartitionSpec as P


MOMENTUM = 0.9
LEARN_RATE = 0.3
F32 = jnp.float32
BF = jnp.bfloat16
MESH = pl.DeviceIdType.MESH
NG = 8
PACK = 4
L = 128
H = 256
W = 512
R = 32
RD = 64
COMM_VMEM = 30 << 20
FINAL_VMEM = 30 << 20
NORM_LAG = 4
SH = 72


def dot(a, b):
    return jnp.dot(a, b, preferred_element_type=F32)


def split3(x):
    a = x.astype(BF)
    r = x - a.astype(F32)
    b = r.astype(BF)
    c = (r - b.astype(F32)).astype(BF)
    return a, b, c


def iota(shape, axis):
    return lax.broadcasted_iota(jnp.int32, shape, axis)


def row_factor(pieces, count, v, rank):
    v1, v2, v3 = split3(v)
    group = iota((1, L), 1) // rank
    acc = acc2 = None
    for m in range(count):
        b12, b1, b3 = pieces(m)
        mask = jnp.where(group == m, 1.0, 0.0).astype(BF)
        w1, w2, w3 = v1 * mask, v2 * mask, v3 * mask
        t = dot(b12, jnp.concatenate([w1, w2], 1))
        u = dot(b1, w3) + dot(b3, w1)
        acc = t if acc is None else acc + t
        acc2 = u if acc2 is None else acc2 + u
    n = acc2.shape[0]
    return acc[:n, :L] + acc2 + (acc[:n, L:] + acc[n:, :L]) + acc[n:, L:]


def col_factor(ut, b1, b2, b3, m, rank):
    lhs = jnp.concatenate([t[rank * m:rank * m + rank] for t in ut], 0)
    o1 = dot(lhs, b1)
    o2 = dot(lhs[:2 * rank], b2)
    o3 = dot(lhs[:rank], b3)
    return o1[:rank] + (o1[rank:2 * rank] + o2[:rank]) + (o1[2 * rank:] + o2[rank:] + o3)


def gram(ut, u, rank):
    full = dot(jnp.concatenate([ut[0], ut[1]], 0), jnp.concatenate([u[0], u[1]], 1))
    low = dot(ut[2], u[0]) + dot(ut[0], u[2])
    g = full[:L, :L] + (full[:L, L:] + full[L:, :L] + low) + full[L:, L:]
    group = iota((rank, L), 1) // rank
    out = jnp.where(group == 0, g[:rank], 0.0)
    for m in range(1, L // rank):
        out = out + jnp.where(group == m, g[rank * m:rank * m + rank], 0.0)
    return out


def inverse_factors(grams, rank):
    lane = iota((rank, L), 1)
    row = iota((rank, L), 0)
    base = (lane // rank) * rank
    col = lane - base
    mats = list(grams)
    for k0 in range(0, rank, 8):
        cols = [[jnp.take_along_axis(a, base + (k0 + j), axis=1) for j in range(8)] for a in mats]
        for j in range(8):
            k = k0 + j
            below = row > k
            for i, a in enumerate(mats):
                ck = cols[i][j]
                factor = jnp.where(below, ck * (1.0 / ck[k:k + 1]), 0.0)
                pivot = jnp.where(col[:1] == k, 1.0, a[k:k + 1])
                mats[i] = jnp.where(below & (col == k), 0.0, a) - factor * pivot
                for l in range(j + 1, 8):
                    cl = cols[i][l]
                    cols[i][l] = cl - factor * cl[k:k + 1]
    out = []
    for a in mats:
        diag = jnp.take_along_axis(a, base + row, axis=1)
        unit = jnp.where(col < row, a, jnp.where(col == row, 1.0, 0.0))
        out.append(unit * (1.0 / jnp.sqrt(diag)))
    return out


def block_diag(inv, rank):
    group = iota((rank, L), 1) // rank
    return jnp.concatenate([jnp.where(group == m, inv, 0.0) for m in range(L // rank)], 0)


def times_right(u, t):
    u1, u2, u3 = split3(u)
    t1, t2, t3 = split3(t)
    t12 = jnp.concatenate([t1, t2], 1)
    a = dot(jnp.concatenate([u1, u2], 1), jnp.concatenate([t12, t12], 0))
    b = dot(jnp.concatenate([u1, u3], 1), jnp.concatenate([t3, t1], 0))
    return a[:, :L] + (a[:, L:] + b)


def times_left(b, v):
    b1, b2, b3 = split3(b)
    v1, v2, v3 = split3(v)
    b12 = jnp.concatenate([b1, b2], 1)
    hi = dot(b12, jnp.concatenate([v1, v1], 0))
    lo = dot(b12, jnp.concatenate([v2, v2], 0))
    lo = lo + dot(jnp.concatenate([b1, b3], 1), jnp.concatenate([v3, v1], 0))
    return hi + lo


def sq_rows_to_lanes(v):
    s = v * v
    f = s[:, :L]
    for i in range(1, v.shape[1] // L):
        f = f + s[:, L * i:L * i + L]
    return jnp.broadcast_to(jnp.sum(f.T, 0, keepdims=True), (8, L))


def sq_lanes(u):
    return jnp.broadcast_to(jnp.sum(u * u, 0, keepdims=True), (8, L))


def gram_to_rows(w, half, rank):
    h = rank // 2
    return jnp.concatenate([w[half * h + 8 * i:half * h + 8 * i + 8] for i in range(h // 8)], 1)


def rows_to_gram(halves, rank):
    parts = []
    for x in halves:
        parts.extend([x[:, L * i:L * i + L] for i in range(rank // 16)])
    return jnp.concatenate(parts, 0)


def comm_kernel(gm, gg, gq, um, ug, uq, dm, dg, dq,
                wqm, wqg, wqf, wkm, wkg, wkf, wvm, wvg, wvf, wom, wog, wof,
                b_e, b_d, b_kv, b_qo, e_inv, e_p, e_rt, e_n, d_r, d_pt, d_n,
                kv_inv, kv_p, kv_rt, kv_n, qo_inv, qo_p, qo_rt, qo_n,
                gs_e, gs_d, qs_e, qs_d, gs_kv, qs_kv, gs_qo, qs_qo,
                z_e, z_d, z_kv, z_qo,
                pown, prcv, down, drc1, dxs, dxr, ptf, sown, src1, sxs, sxr, stf, zown, zrcv,
                nown, nrcv, dnown, dnrcv,
                kpo, kpr, kso, ksr, kxs, kxr, kst, kno, knr,
                qpo, qpr, qso, qsr, qxs, qxr, qst, qno, qnr,
                lsem, dsem, send, recv, sends, recvs, sendk, recvk, sendn, recvn):
    tp = lax.axis_index("tp")
    fs = lax.axis_index("fsdp")
    core = lax.rem(fs, 2)
    ypeer = {"tp": 1 - tp}
    sib = {"fsdp": fs + 1 - 2 * core}
    xpeer = {"fsdp": lax.rem(fs + 2, 4)}

    def loads(g):
        s = lax.rem(g, 2)
        e = pl.ds(g * PACK, PACK)
        pairs = [(gm.at[e], b_e.at[0, e]), (gg.at[e], gs_e.at[s, 0]), (gq.at[e], qs_e.at[s, 0]),
                 (um.at[e], b_e.at[1, e]), (ug.at[e], gs_e.at[s, 1]), (uq.at[e], qs_e.at[s, 1])]
        return [pltpu.make_async_copy(a, b, lsem.at[s, i]) for i, (a, b) in enumerate(pairs)]

    def loads_down(g):
        s = lax.rem(g, 2)
        e = pl.ds(g * PACK, PACK)
        pairs = [(dm.at[e], b_d.at[e]), (dg.at[e], gs_d.at[s]), (dq.at[e], qs_d.at[s])]
        return [pltpu.make_async_copy(a, b, lsem.at[s, len(pairs) * 2 + i]) for i, (a, b) in enumerate(pairs)]

    dense_loads = [pltpu.make_async_copy(a, b, dsem.at[i]) for i, (a, b) in enumerate([
        (wkm, b_kv.at[0]), (wkg, gs_kv.at[0]), (wkf, qs_kv.at[0]),
        (wvm, b_kv.at[1]), (wvg, gs_kv.at[1]), (wvf, qs_kv.at[1]),
        (wqm, b_qo.at[0]), (wqg, gs_qo.at[0]), (wqf, qs_qo.at[0]),
        (wom, b_qo.at[1]), (wog, gs_qo.at[1]), (wof, qs_qo.at[1])])]
    for c in dense_loads:
        c.start()

    barrier = pltpu.get_barrier_semaphore()
    fours = [{"fsdp": lax.rem(fs + i, 4)} for i in (1, 2, 3)]
    for dev in [ypeer] + fours:
        pl.semaphore_signal(barrier, inc=1, device_id=dev, device_id_type=MESH)
    pl.semaphore_wait(barrier, 4)

    def remote(src, dst, ss, rs, dev):
        return pltpu.make_async_remote_copy(src_ref=src, dst_ref=dst, send_sem=ss, recv_sem=rs,
                                            device_id=dev, device_id_type=MESH)

    def c_p(g, q):
        return remote(pown.at[lax.rem(g, 2), q], prcv.at[g, q], send.at[q, g], recv.at[q, g], ypeer)

    def c_d1(g):
        return remote(down.at[lax.rem(g, 2), 1 - core], drc1.at[g], send.at[2, g], recv.at[2, g], sib)

    def c_d2(g):
        return remote(dxs.at[lax.rem(g, 2)], dxr.at[g], send.at[3, g], recv.at[3, g], xpeer)

    def c_d3(g):
        return remote(ptf.at[g, core], ptf.at[g, core], send.at[4, g], recv.at[4, g], sib)

    def c_s1(g, q):
        return remote(sown.at[lax.rem(g, 2), 1 - core, q], src1.at[g, q], sends.at[0, q, g], recvs.at[0, q, g], sib)

    def c_s2(g, q):
        return remote(sxs.at[lax.rem(g, 2), q], sxr.at[g, q], sends.at[1, q, g], recvs.at[1, q, g], xpeer)

    def c_s3(g, q):
        return remote(stf.at[g, core, q], stf.at[g, core, q], sends.at[2, q, g], recvs.at[2, q, g], sib)

    def c_z(g):
        return remote(zown.at[lax.rem(g, 2)], zrcv.at[g], send.at[5, g], recv.at[5, g], ypeer)

    def c_n(g):
        return remote(nown.at[g], nrcv.at[g], send.at[6, g], recv.at[6, g], ypeer)

    def c_nd(g):
        return [remote(dnown.at[g], dnrcv.at[g, i], sendn.at[i, g], recvn.at[i, g], fours[i]) for i in range(3)]

    def dense_copies(i, po, pr, so, sr, xs, xr, st, no, nr):
        k = lambda j: (sendk.at[i, j], recvk.at[i, j])
        return (lambda: remote(po, pr, *k(0), ypeer),
                lambda: remote(so.at[1 - core], sr, *k(1), sib),
                lambda: remote(xs, xr, *k(2), xpeer),
                lambda: remote(st.at[core], st.at[core], *k(3), sib),
                lambda: remote(no, nr, *k(4), ypeer))

    kc = dense_copies(0, kpo, kpr, kso, ksr, kxs, kxr, kst, kno, knr)
    qc = dense_copies(1, qpo, qpr, qso, qsr, qxs, qxr, qst, qno, qnr)

    def terms(b_ref, g_ref, z_ref):
        for r0 in range(0, b_ref.shape[0], RD):
            rs = pl.ds(r0, RD)
            b = b_ref[rs]
            if g_ref is not None:
                b = b + g_ref[rs].astype(F32)
                b_ref[rs] = b
            b1, b2, b3 = split3(b)
            z_ref[0, rs] = b1
            z_ref[1, rs] = b2
            z_ref[2, rs] = b3

    def pieces_of(z_ref):
        n, w = z_ref.shape[1:]
        return z_ref[0:2].reshape(2 * n, w), z_ref[0], z_ref[2]

    def stage1(g):
        s = lax.rem(g, 2)
        for c in loads(g):
            c.wait()

        def one(q, _):
            for m in range(PACK):
                terms(b_e.at[q, g * PACK + m], gs_e.at[s, q, m], z_e.at[m])
            v = qs_e[s, q].reshape(L, H).T
            pown[s, q] = row_factor(lambda m: pieces_of(z_e.at[m]), PACK, v, R)
            c_p(g, q).start()
            return 0

        lax.fori_loop(0, 2, one, 0)

    def stage1_down(g):
        s = lax.rem(g, 2)
        for c in loads_down(g):
            c.wait()
        ut = split3(qs_d[s].reshape(L, L))
        for m in range(PACK):
            terms(b_d.at[g * PACK + m], gs_d.at[s, m], z_d.at[m])
            part = col_factor(ut, z_d[m, 0], z_d[m, 1], z_d[m, 2], m, R)
            down[s, 0, pl.ds(R * m, R)] = part[:, :H]
            down[s, 1, pl.ds(R * m, R)] = part[:, H:]
        c_d1(g).start()

    low = iota((1, L), 1) < RD

    def stage1_dense():
        for c in dense_loads[:6]:
            c.wait()
        for i in range(2):
            terms(b_kv.at[i], gs_kv.at[i], z_kv.at[i])
        v = jnp.concatenate([qs_kv[0], qs_kv[1], qs_kv[0], qs_kv[1]], 0).T
        u = row_factor(lambda m: pieces_of(z_kv.at[m % 2]), 4, v, R)
        kpo[:] = jnp.where(low, u[:L], u[L:])
        kc[0]().start()
        for c in dense_loads[6:]:
            c.wait()
        for c in loads_down(0) + loads(0) + loads_down(1):
            c.start()
        for i in range(2):
            terms(b_qo.at[i], gs_qo.at[i], z_qo.at[i])
        v = qs_qo[:].reshape(L, W).T
        qpo[:] = row_factor(lambda m: pieces_of(z_qo.at[m]), 2, v, RD)
        qc[0]().start()

    def stage2a(g):
        s = lax.rem(g, 2)
        c_d1(g).wait()
        dxs[s] = down[s, core] + drc1[g]
        c_d2(g).start()

    def stage2b(g):
        c_d2(g).wait()
        ptf[g, core] = dxs[lax.rem(g, 2)] + dxr[g]
        c_d3(g).start()

    def s_and_gram(u, rank, count, z_of, so):
        ut = u.T
        up, utp = split3(u), split3(ut)
        half = L // rank // 2
        for m in range(count):
            z = z_of(m)
            so[m // half, pl.ds(rank * (m % half), rank)] = col_factor(utp, z[0], z[1], z[2], m, rank)
        w = gram(utp, up, rank)
        for h in range(2):
            so[h, pl.ds(RD, 8)] = gram_to_rows(w, h, rank)

    def stage2c(g):
        s = lax.rem(g, 2)

        def one(q, _):
            c_p(g, q).wait()
            u = pown[s, q] + prcv[g, q]
            e_p[g, q] = u
            for m in range(PACK):
                terms(b_e.at[q, g * PACK + m], None, z_e.at[m])
            s_and_gram(u, R, PACK, z_e.at.__getitem__, sown.at[s, :, q])
            c_s1(g, q).start()
            return 0

        lax.fori_loop(0, 2, one, 0)

    def stage2c_down(g):
        s = lax.rem(g, 2)
        for m in range(PACK):
            terms(b_d.at[g * PACK + m], None, z_d.at[m])
        c_d3(g).wait()
        vt = jnp.concatenate([ptf[g, 0], ptf[g, 1]], 1)
        d_pt[g] = vt
        v = vt.T
        zown[s, pl.ds(0, L)] = row_factor(lambda m: pieces_of(z_d.at[m]), PACK, v, R)
        zown[s, pl.ds(L, R)] = gram(split3(vt), split3(v), R)
        c_z(g).start()

    def stage2_dense():
        kc[0]().wait()
        u = kpo[:] + kpr[:]
        t = pltpu.roll(u, RD, 1)
        u = jnp.concatenate([jnp.where(low, u, t), jnp.where(low, t, u)], 0)
        kv_p[:] = u
        s_and_gram(u, R, 4, lambda m: z_kv.at[m % 2], kso)
        kc[1]().start()
        qc[0]().wait()
        u = qpo[:] + qpr[:]
        qo_p[:] = u
        s_and_gram(u, RD, 2, lambda m: z_qo.at[m], qso)
        qc[1]().start()

    def stage3a(g, q):
        s = lax.rem(g, 2)
        c_s1(g, q).wait()
        sxs[s, q] = sown[s, core, q] + src1[g, q]
        c_s2(g, q).start()

    def stage3b(g):
        for q in range(2):
            c_s2(g, q).wait()
            stf[g, core, q] = sxs[lax.rem(g, 2), q] + sxr[g, q]
            c_s3(g, q).start()

    def stage3a_dense():
        for cs, so, sr, xs in ((kc, kso, ksr, kxs), (qc, qso, qsr, qxs)):
            cs[1]().wait()
            xs[:] = so[core] + sr[:]
            cs[2]().start()

    def stage3b_dense():
        for cs, xs, xr, st in ((kc, kxs, kxr, kst), (qc, qxs, qxr, qst)):
            cs[2]().wait()
            st[core] = xs[:] + xr[:]
            cs[3]().start()

    def apply_keep(rt_ref, n_ref, inv, st, rank):
        bd = block_diag(inv, rank)
        vt = jnp.concatenate([st[0, pl.ds(0, RD)], st[1, pl.ds(0, RD)]], 0)
        rt = times_left(bd, vt)
        rt_ref[:] = rt
        n_ref[:] = sq_rows_to_lanes(rt)

    def stage4(g):
        s = lax.rem(g, 2)
        for q in range(2):
            c_s3(g, q).wait()
        c_z(g).wait()
        z = zown[s] + zrcv[g]
        ws = [rows_to_gram([stf[g, h, q, pl.ds(RD, 8)] for h in range(2)], R) for q in range(2)]
        inv = inverse_factors(ws + [z[L:]], R)
        for i in range(3):
            e_inv[g, i] = inv[i]
        for q in range(2):
            apply_keep(e_rt.at[g, q], nown.at[g, q], inv[q], stf.at[g, :, q], R)
        c_n(g).start()
        bd = block_diag(inv[2], R)
        r = times_right(z[:L], bd.T)
        d_r[g] = r
        dnown[g] = sq_lanes(r)
        for c in c_nd(g):
            c.start()

    def stage4_dense():
        kc[3]().wait()
        inv = inverse_factors([rows_to_gram([kst[h, pl.ds(RD, 8)] for h in range(2)], R)], R)
        kv_inv[:] = inv[0]
        apply_keep(kv_rt, kno, inv[0], kst, R)
        kc[4]().start()
        qc[3]().wait()
        inv = inverse_factors([rows_to_gram([qst[h, pl.ds(RD, 8)] for h in range(2)], RD)], RD)
        qo_inv[:] = inv[0]
        apply_keep(qo_rt, qno, inv[0], qst, RD)
        qc[4]().start()

    def stage5(g):
        c_n(g).wait()
        for q in range(2):
            e_n[g, q] = 1.0 / jnp.sqrt(nown[g, q] + nrcv[g, q])
        for c in c_nd(g):
            c.wait()
        d_n[g] = 1.0 / jnp.sqrt((dnown[g] + dnrcv[g, 1]) + (dnrcv[g, 0] + dnrcv[g, 2]))

    def stage5_dense():
        kc[4]().wait()
        kv_n[:] = 1.0 / jnp.sqrt(kno[:] + knr[:])
        qc[4]().wait()
        qo_n[:] = 1.0 / jnp.sqrt(qno[:] + qnr[:])

    stage1_dense()
    stage1_down(0)

    def step(t, _):
        def within(lag, stage):
            @pl.when((t >= lag) & (t < NG + lag))
            def _():
                stage(t - lag)

        def only(at, stage):
            @pl.when(t == at)
            def _():
                stage()

        @pl.when(t < NG - 1)
        def _():
            for c in loads(t + 1):
                c.start()

        @pl.when(t < NG - 2)
        def _():
            for c in loads_down(t + 2):
                c.start()

        within(0, stage2a)
        within(0, stage1)

        @pl.when(t < NG - 1)
        def _():
            stage1_down(t + 1)

        within(1, stage2b)
        within(NORM_LAG, stage5)
        only(3, stage5_dense)
        only(0, stage2_dense)
        within(1, stage2c)
        within(1, lambda g: stage3a(g, 0))
        within(2, stage3b)
        only(1, stage3b_dense)
        within(1, stage2c_down)
        within(1, lambda g: stage3a(g, 1))
        only(0, stage3a_dense)
        within(2, stage4)
        only(1, stage4_dense)
        return 0

    lax.fori_loop(0, NG + 2, step, 0)
    for g in range(NG + 2 - NORM_LAG, NG):
        stage5(g)


def run_comm(args):
    v = pltpu.VMEM
    dma = pltpu.SemaphoreType.DMA
    out = lambda *shape: v(shape, F32)
    out_shape = [out(2, R, H, H), out(R, L, W), out(2, H, H), out(2, H, W),
                 out(NG, 3, R, L), out(NG, 2, H, L), out(NG, 2, L, H), out(NG, 2, 8, L),
                 out(NG, L, L), out(NG, L, W), out(NG, 8, L),
                 out(R, L), out(H, L), out(L, H), out(8, L),
                 out(RD, L), out(H, L), out(L, W), out(8, L)]

    def pack_bufs(rows, w):
        return [v((rows, L), F32), v((rows, L), F32), v((2, SH, w), F32), v((SH, w), F32), v((SH, w), F32),
                v((SH, w), F32), v((2, SH, w), F32), v((8, L), F32), v((8, L), F32)]

    scratch = [
        v((2, 2, 4, H, H), BF), v((2, 4, L, W), BF), v((2, 2, 4, R, H), F32), v((2, 4, R, L), F32),
        v((2, H, H), BF), v((2, R, H), F32), v((2, H, W), BF), v((2, RD, W), F32),
        v((4, 3, H, H), BF), v((4, 3, L, W), BF), v((2, 3, H, H), BF), v((2, 3, H, W), BF),
        v((2, 2, H, L), F32), v((NG, 2, H, L), F32),
        v((2, 2, L, H), F32), v((NG, L, H), F32), v((2, L, H), F32), v((NG, L, H), F32),
        v((NG, 2, L, H), F32),
        v((2, 2, 2, SH, H), F32), v((NG, 2, SH, H), F32), v((2, 2, SH, H), F32), v((NG, 2, SH, H), F32),
        v((NG, 2, 2, SH, H), F32),
        v((2, 160, L), F32), v((NG, 160, L), F32),
        v((NG, 2, 8, L), F32), v((NG, 2, 8, L), F32), v((NG, 8, L), F32), v((NG, 3, 8, L), F32),
    ] + pack_bufs(L, H) + pack_bufs(H, W) + [
        dma((2, 9)), dma((12,)), dma((7, NG)), dma((7, NG)), dma((3, 2, NG)), dma((3, 2, NG)), dma((2, 5)), dma((2, 5)), dma((3, NG)), dma((3, NG))]
    return pl.pallas_call(
        comm_kernel,
        out_shape=out_shape,
        in_specs=[pl.BlockSpec(memory_space=pl.ANY)] * 21,
        out_specs=[pl.BlockSpec(memory_space=pltpu.VMEM)] * len(out_shape),
        scratch_shapes=scratch,
        name="comm_kernel",
        compiler_params=pltpu.CompilerParams(collective_id=0, has_side_effects=True, vmem_limit_bytes=COMM_VMEM),
    )(*args)


def lane_copies(u, rank):
    count = L // rank
    group = iota((1, L), 1) // rank
    rolled = [u] + [pltpu.roll(u, rank * s, 1) for s in range(1, count)]
    outs = []
    for m in range(count):
        x = rolled[(0 - m) % count]
        for gidx in range(1, count):
            x = jnp.where(group == gidx, rolled[(gidx - m) % count], x)
        outs.append(x)
    return outs


def left_tiles(x, rank):
    a = x.astype(BF)
    r1 = x - a.astype(F32)
    b = r1.astype(BF)
    r2 = r1 - b.astype(F32)
    low = iota((1, L), 1) < RD
    if rank == R:
        return jnp.concatenate([a, jnp.where(low, r1, r2).astype(BF)], 1)
    return jnp.concatenate([a, jnp.where(low, x, r1).astype(BF), jnp.where(low, r1, r2).astype(BF)], 1)


def right_tiles(vt, rank):
    a, b, c = split3(vt)
    if rank == R:
        return jnp.concatenate([a, b, c, jnp.zeros_like(a), a, b, a, b], 0)
    return jnp.concatenate([a, b, c, a, b, a], 0)


def lanes_to_rows(n):
    return jnp.broadcast_to(n[:1], (L, L)).T


def scale_rows(vt, n):
    t = lanes_to_rows(n)
    return jnp.concatenate([vt[:, L * i:L * i + L] * t for i in range(vt.shape[1] // L)], 1)


def keep_update(p0, inv, rt, n, rank, slots, x_of, b_of, xo, mo, qo, step):
    copies = lane_copies(times_right(p0, block_diag(inv, rank).T), rank)
    rts = scale_rows(rt, n)
    for m in slots:
        lhs = left_tiles(copies[m], rank)
        rows = slice(rank * m, rank * m + rank)
        both = right_tiles(jnp.concatenate([rt[rows] * (1.0 - MOMENTUM), rts[rows] * step], 1), rank)
        out = dot(lhs, both)
        n_cols = rt.shape[1]
        mo(m)[:] = b_of(m)[:] - out[:, :n_cols]
        xo(m)[:] = x_of(m)[:] - out[:, n_cols:]
        qo(m)[:] = rts[rows]


def final_kernel(gx, ux, dx, qx, kx, vx, ox,
                 b_e, b_d, b_kv, b_qo, e_inv, e_p, e_rt, e_n, d_r, d_pt, d_n,
                 kv_inv, kv_p, kv_rt, kv_n, qo_inv, qo_p, qo_rt, qo_n,
                 gxo, gmo, gqo, uxo, umo, uqo, dxo, dmo, dqo,
                 qxo, qmo, qqo, kxo, kmo, kqo, vxo, vmo, vqo, oxo, omo, oqo,
                 xs_kv, xs_qo, mt_kv, mt_qo, qt_kv, qt_qo, isem, osem):
    i = pl.program_id(0)
    step = LEARN_RATE * math.sqrt(2.0)
    ins = [pltpu.make_async_copy(a, b, isem.at[k]) for k, (a, b) in enumerate(
        [(kx, xs_kv.at[0]), (vx, xs_kv.at[1]), (qx, xs_qo.at[0]), (ox, xs_qo.at[1])])]
    outs = [pltpu.make_async_copy(b, a, osem.at[k]) for k, (a, b) in enumerate(
        [(kxo, xs_kv.at[0]), (vxo, xs_kv.at[1]), (qxo, xs_qo.at[0]), (oxo, xs_qo.at[1]),
         (kmo, mt_kv.at[0]), (vmo, mt_kv.at[1]), (qmo, mt_qo.at[0]), (omo, mt_qo.at[1]),
         (kqo, qt_kv.at[0]), (vqo, qt_kv.at[1]), (qqo, qt_qo.at[0]), (oqo, qt_qo.at[1])])]

    @pl.when(i == 0)
    def _():
        for c in ins:
            c.start()

    for q, (x, xo, mo, qo) in enumerate(((gx, gxo, gmo, gqo), (ux, uxo, umo, uqo))):
        keep_update(e_p[i, q], e_inv[i, q], e_rt[i, q], e_n[i, q], R, range(PACK),
                    x.at.__getitem__, lambda m: b_e.at[q, i * PACK + m],
                    xo.at.__getitem__, mo.at.__getitem__, qo.at.__getitem__, step)
    r = d_r[i]
    pt = times_left(block_diag(e_inv[i, 2], R), d_pt[i])
    qpack = r * d_n[i][:1]
    rcopies = lane_copies(r * (1.0 - MOMENTUM), R)
    qcopies = lane_copies(qpack * step, R)
    qrows = qpack.T
    for m in range(PACK):
        rhs = right_tiles(pt[R * m:R * m + R], R)
        out = dot(jnp.concatenate([left_tiles(rcopies[m], R), left_tiles(qcopies[m], R)], 0), rhs)
        dmo[m] = b_d[i * PACK + m] - out[:L]
        dxo[m] = dx[m] - out[L:]
        dqo[m] = qrows[R * m:R * m + R]

    @pl.when(i == 1)
    def _():
        for c in ins:
            c.wait()
        keep_update(kv_p[:], kv_inv[:], kv_rt[:], kv_n[:], R, range(2),
                    xs_kv.at.__getitem__, b_kv.at.__getitem__,
                    xs_kv.at.__getitem__, mt_kv.at.__getitem__, qt_kv.at.__getitem__, step)
        keep_update(qo_p[:], qo_inv[:], qo_rt[:], qo_n[:], RD, range(2),
                    xs_qo.at.__getitem__, b_qo.at.__getitem__,
                    xs_qo.at.__getitem__, mt_qo.at.__getitem__, qt_qo.at.__getitem__, LEARN_RATE)
        for c in outs:
            c.start()

    @pl.when(i == NG - 1)
    def _():
        for c in outs:
            c.wait()


def run_final(xs, packs):
    hbm = pl.BlockSpec(memory_space=pl.ANY)
    v = pltpu.VMEM

    def spec(a):
        return pl.BlockSpec((PACK,) + a.shape[1:], lambda i: (i, 0, 0))

    out = lambda *shape: jax.ShapeDtypeStruct(shape, F32)
    big = [out(R, H, H), out(R, H, H), out(R, R, H)]
    stacks = big + big + [out(R, L, W), out(R, L, W), out(R, R, L)]
    wide = [out(H, W), out(H, W), out(RD, W)]
    narrow = [out(H, H), out(H, H), out(R, H)]
    return pl.pallas_call(
        final_kernel,
        grid=(NG,),
        out_shape=stacks + wide + narrow + narrow + wide,
        in_specs=[spec(a) for a in xs[:3]] + [hbm] * 4 + [pl.BlockSpec(memory_space=v)] * len(packs),
        out_specs=[spec(a) for a in stacks] + [hbm] * 12,
        scratch_shapes=[v((2, H, H), F32), v((2, H, W), F32), v((2, H, H), F32), v((2, H, W), F32),
                        v((2, R, H), F32), v((2, RD, W), F32),
                        pltpu.SemaphoreType.DMA((4,)), pltpu.SemaphoreType.DMA((12,))],
        name="final_kernel",
        compiler_params=pltpu.CompilerParams(vmem_limit_bytes=FINAL_VMEM, dimension_semantics=("arbitrary",)),
    )(*xs, *packs)


def solution(mesh):
    dense_w = P(('layer', 'fsdp'), 'tp')
    dense_f = P(('layer', 'tp'), None)
    stack_w = P('layer', 'fsdp', 'tp')
    stack_f = P('layer', 'tp', None)
    down_f = P('layer', 'fsdp', None)
    in_specs = (dense_w, dense_w, dense_w, dense_f) * 4 + (stack_w, stack_w, stack_w, stack_f) * 2 + (stack_w, stack_w, stack_w, down_f)
    out_specs = (dense_w, dense_w, dense_f) * 4 + (stack_w, stack_w, stack_f) * 2 + (stack_w, stack_w, down_f)

    def local_step(*b):
        x, m, g = b[0::4], b[1::4], b[2::4]
        q = [jnp.swapaxes(f, -1, -2) for f in b[3::4]]
        comm_in = []
        for i in (4, 5, 6, 0, 1, 2, 3):
            comm_in += [m[i], g[i], q[i]]
        packs = [pltpu.with_memory_space_constraint(a, pltpu.VMEM) for a in run_comm(comm_in)]
        outs = run_final([x[i] for i in (4, 5, 6, 0, 1, 2, 3)], packs)
        outs = list(outs[9:]) + list(outs[:9])
        for i in range(2, 21, 3):
            outs[i] = jnp.swapaxes(outs[i], -1, -2)
        return tuple(outs)

    return jax.shard_map(local_step, mesh=mesh, in_specs=in_specs, out_specs=out_specs, check_vma=False)
```

```python
import math
import jax
import jax.numpy as jnp
from jax import lax
from jax.experimental import pallas as pl
from jax.experimental.pallas import tpu as pltpu
from jax.sharding import PartitionSpec as P


MOMENTUM = 0.9
LEARN_RATE = 0.3
F32 = jnp.float32
BF = jnp.bfloat16
MESH = pl.DeviceIdType.MESH
NG = 8
PACK = 4
L = 128
H = 256
W = 512
R = 32
RD = 64
COMM_VMEM = 22 << 20
FINAL_VMEM = 22 << 20
NORM_LAG = 4
OUT_SLOTS = 3
IN_SLOTS = 4
TWO = 2
SH = 72


def dot(a, b):
    return jnp.dot(a, b, preferred_element_type=F32)


def split3(x):
    a = x.astype(BF)
    r = x - a.astype(F32)
    b = r.astype(BF)
    c = (r - b.astype(F32)).astype(BF)
    return a, b, c


def iota(shape, axis):
    return lax.broadcasted_iota(jnp.int32, shape, axis)


def row_factor(pieces, count, v, rank):
    v1, v2, v3 = split3(v)
    group = iota((1, L), 1) // rank
    acc = acc2 = None
    for m in range(count):
        b12, b1, b3 = pieces(m)
        mask = jnp.where(group == m, 1.0, 0.0).astype(BF)
        w1, w2, w3 = v1 * mask, v2 * mask, v3 * mask
        t = dot(b12, jnp.concatenate([w1, w2], 1))
        u = dot(b1, w3) + dot(b3, w1)
        acc = t if acc is None else acc + t
        acc2 = u if acc2 is None else acc2 + u
    n = acc2.shape[0]
    return acc[:n, :L] + acc2 + (acc[:n, L:] + acc[n:, :L]) + acc[n:, L:]


def col_factor(ut, b1, b2, b3, m, rank):
    lhs = jnp.concatenate([t[rank * m:rank * m + rank] for t in ut], 0)
    o1 = dot(lhs, b1)
    o2 = dot(lhs[:2 * rank], b2)
    o3 = dot(lhs[:rank], b3)
    return o1[:rank] + (o1[rank:2 * rank] + o2[:rank]) + (o1[2 * rank:] + o2[rank:] + o3)


def gram(ut, u, rank):
    full = dot(jnp.concatenate([ut[0], ut[1]], 0), jnp.concatenate([u[0], u[1]], 1))
    low = dot(ut[2], u[0]) + dot(ut[0], u[2])
    g = full[:L, :L] + (full[:L, L:] + full[L:, :L] + low) + full[L:, L:]
    group = iota((rank, L), 1) // rank
    out = jnp.where(group == 0, g[:rank], 0.0)
    for m in range(1, L // rank):
        out = out + jnp.where(group == m, g[rank * m:rank * m + rank], 0.0)
    return out


def inverse_factors(grams, rank):
    lane = iota((rank, L), 1)
    row = iota((rank, L), 0)
    base = (lane // rank) * rank
    col = lane - base
    mats = list(grams)
    for k0 in range(0, rank, 8):
        cols = [[jnp.take_along_axis(a, base + (k0 + j), axis=1) for j in range(8)] for a in mats]
        for j in range(8):
            k = k0 + j
            below = row > k
            for i, a in enumerate(mats):
                ck = cols[i][j]
                factor = jnp.where(below, ck * (1.0 / ck[k:k + 1]), 0.0)
                pivot = jnp.where(col[:1] == k, 1.0, a[k:k + 1])
                mats[i] = jnp.where(below & (col == k), 0.0, a) - factor * pivot
                for l in range(j + 1, 8):
                    cl = cols[i][l]
                    cols[i][l] = cl - factor * cl[k:k + 1]
    out = []
    for a in mats:
        diag = jnp.take_along_axis(a, base + row, axis=1)
        unit = jnp.where(col < row, a, jnp.where(col == row, 1.0, 0.0))
        out.append(unit * (1.0 / jnp.sqrt(diag)))
    return out


def block_diag(inv, rank):
    group = iota((rank, L), 1) // rank
    return jnp.concatenate([jnp.where(group == m, inv, 0.0) for m in range(L // rank)], 0)


def times_right(u, t):
    u1, u2, u3 = split3(u)
    t1, t2, t3 = split3(t)
    t12 = jnp.concatenate([t1, t2], 1)
    a = dot(jnp.concatenate([u1, u2], 1), jnp.concatenate([t12, t12], 0))
    b = dot(jnp.concatenate([u1, u3], 1), jnp.concatenate([t3, t1], 0))
    return a[:, :L] + (a[:, L:] + b)


def times_left(b, v):
    b1, b2, b3 = split3(b)
    v1, v2, v3 = split3(v)
    b12 = jnp.concatenate([b1, b2], 1)
    hi = dot(b12, jnp.concatenate([v1, v1], 0))
    lo = dot(b12, jnp.concatenate([v2, v2], 0))
    lo = lo + dot(jnp.concatenate([b1, b3], 1), jnp.concatenate([v3, v1], 0))
    return hi + lo


def sq_rows_to_lanes(v):
    s = v * v
    f = s[:, :L]
    for i in range(1, v.shape[1] // L):
        f = f + s[:, L * i:L * i + L]
    return jnp.broadcast_to(jnp.sum(f.T, 0, keepdims=True), (8, L))


def sq_lanes(u):
    return jnp.broadcast_to(jnp.sum(u * u, 0, keepdims=True), (8, L))


def gram_to_rows(w, half, rank):
    h = rank // 2
    return jnp.concatenate([w[half * h + 8 * i:half * h + 8 * i + 8] for i in range(h // 8)], 1)


def rows_to_gram(halves, rank):
    parts = []
    for x in halves:
        parts.extend([x[:, L * i:L * i + L] for i in range(rank // 16)])
    return jnp.concatenate(parts, 0)


def comm_kernel(gm, gg, gq, um, ug, uq, dm, dg, dq,
                wqm, wqg, wqf, wkm, wkg, wkf, wvm, wvg, wvf, wom, wog, wof, gx,
                x_g, b_e, b_d, b_kv, b_qo, e_inv, e_p, e_rt, e_n, d_r, d_pt, d_n,
                kv_inv, kv_p, kv_rt, kv_n, qo_inv, qo_p, qo_rt, qo_n,
                gs_e, gs_d, qs_e, qs_d, gs_kv, qs_kv, gs_qo, qs_qo,
                z_e, z_d, z_kv, z_qo,
                pown, prcv, down, drc1, dxs, dxr, sown, src1, sxs, sxr, stf, zown, zrcv,
                nown, nrcv, dnown, dnrcv,
                kpo, kpr, kso, ksr, kxs, kxr, kst, kno, knr,
                qpo, qpr, qso, qsr, qxs, qxr, qst, qno, qnr,
                lsem, dsem, send, recv, sends, recvs, sendk, recvk, sendn, recvn):
    tp = lax.axis_index("tp")
    fs = lax.axis_index("fsdp")
    core = lax.rem(fs, 2)
    ypeer = {"tp": 1 - tp}
    sib = {"fsdp": fs + 1 - 2 * core}
    xpeer = {"fsdp": lax.rem(fs + 2, 4)}

    def loads(g):
        s = lax.rem(g, 2)
        e = pl.ds(g * PACK, PACK)
        pairs = [(gm.at[e], b_e.at[0, e]), (gg.at[e], gs_e.at[s, 0]), (gq.at[e], qs_e.at[s, 0]),
                 (um.at[e], b_e.at[1, e]), (ug.at[e], gs_e.at[s, 1]), (uq.at[e], qs_e.at[s, 1])]
        return [pltpu.make_async_copy(a, b, lsem.at[s, i]) for i, (a, b) in enumerate(pairs)]

    def loads_down(g):
        s = lax.rem(g, 2)
        e = pl.ds(g * PACK, PACK)
        pairs = [(dm.at[e], b_d.at[e]), (dg.at[e], gs_d.at[s]), (dq.at[e], qs_d.at[s])]
        return [pltpu.make_async_copy(a, b, lsem.at[s, len(pairs) * 2 + i]) for i, (a, b) in enumerate(pairs)]

    dense_loads = [pltpu.make_async_copy(a, b, dsem.at[i]) for i, (a, b) in enumerate([
        (wkm, b_kv.at[0]), (wkg, gs_kv.at[0]), (wkf, qs_kv.at[0]),
        (wvm, b_kv.at[1]), (wvg, gs_kv.at[1]), (wvf, qs_kv.at[1]),
        (wqm, b_qo.at[0]), (wqg, gs_qo.at[0]), (wqf, qs_qo.at[0]),
        (wom, b_qo.at[1]), (wog, gs_qo.at[1]), (wof, qs_qo.at[1])])]
    x_load = pltpu.make_async_copy(gx, x_g, dsem.at[len(dense_loads)])
    for c in dense_loads:
        c.start()

    barrier = pltpu.get_barrier_semaphore()
    fours = [{"fsdp": lax.rem(fs + i, 4)} for i in (1, 2, 3)]
    for dev in [ypeer] + fours:
        pl.semaphore_signal(barrier, inc=1, device_id=dev, device_id_type=MESH)
    pl.semaphore_wait(barrier, 4)

    def remote(src, dst, ss, rs, dev):
        return pltpu.make_async_remote_copy(src_ref=src, dst_ref=dst, send_sem=ss, recv_sem=rs,
                                            device_id=dev, device_id_type=MESH)

    def c_p(g, q):
        return remote(pown.at[lax.rem(g, 2), q], prcv.at[lax.rem(g, 3), q], send.at[q, g], recv.at[q, g], ypeer)

    def c_d1(g):
        return remote(down.at[lax.rem(g, 2), 1 - core], drc1.at[lax.rem(g, 2)], send.at[2, g], recv.at[2, g], sib)

    def c_d2(g):
        return remote(dxs.at[lax.rem(g, 2)], dxr.at[lax.rem(g, 3)], send.at[3, g], recv.at[3, g], xpeer)

    def c_d3(g):
        return remote(d_pt.at[g, core], d_pt.at[g, core], send.at[4, g], recv.at[4, g], sib)

    def c_s1(g, q):
        return remote(sown.at[lax.rem(g, 2), 1 - core, q], src1.at[lax.rem(g, 2), q], sends.at[0, q, g], recvs.at[0, q, g], sib)

    def c_s2(g, q):
        return remote(sxs.at[lax.rem(g, 2), q], sxr.at[lax.rem(g, 3), q], sends.at[1, q, g], recvs.at[1, q, g], xpeer)

    def c_s3(g, q):
        return remote(stf.at[lax.rem(g, 2), core, q], stf.at[lax.rem(g, 2), core, q], sends.at[2, q, g], recvs.at[2, q, g], sib)

    def c_z(g):
        return remote(zown.at[lax.rem(g, 2)], zrcv.at[lax.rem(g, 3)], send.at[5, g], recv.at[5, g], ypeer)

    def c_n(g):
        return remote(nown.at[g], nrcv.at[g], send.at[6, g], recv.at[6, g], ypeer)

    def c_nd(g):
        return [remote(dnown.at[g], dnrcv.at[g, i], sendn.at[i, g], recvn.at[i, g], fours[i]) for i in range(3)]

    def dense_copies(i, po, pr, so, sr, xs, xr, st, no, nr):
        k = lambda j: (sendk.at[i, j], recvk.at[i, j])
        return (lambda: remote(po, pr, *k(0), ypeer),
                lambda: remote(so.at[1 - core], sr, *k(1), sib),
                lambda: remote(xs, xr, *k(2), xpeer),
                lambda: remote(st.at[core], st.at[core], *k(3), sib),
                lambda: remote(no, nr, *k(4), ypeer))

    kc = dense_copies(0, kpo, kpr, kso, ksr, kxs, kxr, kst, kno, knr)
    qc = dense_copies(1, qpo, qpr, qso, qsr, qxs, qxr, qst, qno, qnr)

    def terms(b_ref, g_ref, z_ref):
        for r0 in range(0, b_ref.shape[0], RD):
            rs = pl.ds(r0, RD)
            b = b_ref[rs]
            if g_ref is not None:
                b = b + g_ref[rs].astype(F32)
                b_ref[rs] = b
            b1, b2, b3 = split3(b)
            z_ref[0, rs] = b1
            z_ref[1, rs] = b2
            z_ref[2, rs] = b3

    def pieces_of(z_ref):
        n, w = z_ref.shape[1:]
        return z_ref[0:2].reshape(2 * n, w), z_ref[0], z_ref[2]

    def stage1(g):
        s = lax.rem(g, 2)
        for c in loads(g):
            c.wait()

        def one(q, _):
            for m in range(PACK):
                terms(b_e.at[q, g * PACK + m], gs_e.at[s, q, m], z_e.at[m])
            v = qs_e[s, q].reshape(L, H).T
            pown[s, q] = row_factor(lambda m: pieces_of(z_e.at[m]), PACK, v, R)
            c_p(g, q).start()
            return 0

        lax.fori_loop(0, 2, one, 0)

    def stage1_down(g):
        s = lax.rem(g, 2)
        for c in loads_down(g):
            c.wait()
        ut = split3(qs_d[s].reshape(L, L))
        for m in range(PACK):
            terms(b_d.at[g * PACK + m], gs_d.at[s, m], z_d.at[m])
            part = col_factor(ut, z_d[m, 0], z_d[m, 1], z_d[m, 2], m, R)
            down[s, 0, pl.ds(R * m, R)] = part[:, :H]
            down[s, 1, pl.ds(R * m, R)] = part[:, H:]
        c_d1(g).start()

    low = iota((1, L), 1) < RD

    def stage1_dense():
        for c in dense_loads[:6]:
            c.wait()
        for i in range(2):
            terms(b_kv.at[i], gs_kv.at[i], z_kv.at[i])
        v = jnp.concatenate([qs_kv[0], qs_kv[1], qs_kv[0], qs_kv[1]], 0).T
        u = row_factor(lambda m: pieces_of(z_kv.at[m % 2]), 4, v, R)
        kpo[:] = jnp.where(low, u[:L], u[L:])
        kc[0]().start()
        for c in dense_loads[6:]:
            c.wait()
        for c in loads_down(0) + loads(0) + loads_down(1):
            c.start()
        for i in range(2):
            terms(b_qo.at[i], gs_qo.at[i], z_qo.at[i])
        v = qs_qo[:].reshape(L, W).T
        qpo[:] = row_factor(lambda m: pieces_of(z_qo.at[m]), 2, v, RD)
        qc[0]().start()

    def stage2a(g):
        s = lax.rem(g, 2)
        c_d1(g).wait()
        dxs[s] = down[s, core] + drc1[s]
        c_d2(g).start()

    def stage2b(g):
        c_d2(g).wait()
        d_pt[g, core] = dxs[lax.rem(g, 2)] + dxr[lax.rem(g, 3)]
        c_d3(g).start()

    def s_and_gram(u, rank, count, z_of, so):
        ut = u.T
        up, utp = split3(u), split3(ut)
        half = L // rank // 2
        for m in range(count):
            z = z_of(m)
            so[m // half, pl.ds(rank * (m % half), rank)] = col_factor(utp, z[0], z[1], z[2], m, rank)
        w = gram(utp, up, rank)
        for h in range(2):
            so[h, pl.ds(RD, 8)] = gram_to_rows(w, h, rank)

    def stage2c(g):
        s = lax.rem(g, 2)

        def one(q, _):
            c_p(g, q).wait()
            u = pown[s, q] + prcv[lax.rem(g, 3), q]
            e_p[g, q] = u
            for m in range(PACK):
                terms(b_e.at[q, g * PACK + m], None, z_e.at[m])
            s_and_gram(u, R, PACK, z_e.at.__getitem__, sown.at[s, :, q])
            c_s1(g, q).start()
            return 0

        lax.fori_loop(0, 2, one, 0)

    def stage2c_down(g):
        s = lax.rem(g, 2)
        for m in range(PACK):
            terms(b_d.at[g * PACK + m], None, z_d.at[m])
        c_d3(g).wait()
        vt = jnp.concatenate([d_pt[g, 0], d_pt[g, 1]], 1)
        v = vt.T
        zown[s, pl.ds(0, L)] = row_factor(lambda m: pieces_of(z_d.at[m]), PACK, v, R)
        zown[s, pl.ds(L, R)] = gram(split3(vt), split3(v), R)
        c_z(g).start()

    def stage2_dense():
        kc[0]().wait()
        u = kpo[:] + kpr[:]
        t = pltpu.roll(u, RD, 1)
        u = jnp.concatenate([jnp.where(low, u, t), jnp.where(low, t, u)], 0)
        kv_p[:] = u
        s_and_gram(u, R, 4, lambda m: z_kv.at[m % 2], kso)
        kc[1]().start()
        qc[0]().wait()
        u = qpo[:] + qpr[:]
        qo_p[:] = u
        s_and_gram(u, RD, 2, lambda m: z_qo.at[m], qso)
        qc[1]().start()

    def stage3a(g, q):
        s = lax.rem(g, 2)
        c_s1(g, q).wait()
        sxs[s, q] = sown[s, core, q] + src1[s, q]
        c_s2(g, q).start()

    def stage3b(g):
        for q in range(2):
            c_s2(g, q).wait()
            stf[lax.rem(g, 2), core, q] = sxs[lax.rem(g, 2), q] + sxr[lax.rem(g, 3), q]
            c_s3(g, q).start()

    def stage3a_dense():
        for cs, so, sr, xs in ((kc, kso, ksr, kxs), (qc, qso, qsr, qxs)):
            cs[1]().wait()
            xs[:] = so[core] + sr[:]
            cs[2]().start()

    def stage3b_dense():
        for cs, xs, xr, st in ((kc, kxs, kxr, kst), (qc, qxs, qxr, qst)):
            cs[2]().wait()
            st[core] = xs[:] + xr[:]
            cs[3]().start()

    def apply_keep(rt_ref, n_ref, inv, st, rank):
        bd = block_diag(inv, rank)
        vt = jnp.concatenate([st[0, pl.ds(0, RD)], st[1, pl.ds(0, RD)]], 0)
        rt = times_left(bd, vt)
        rt_ref[:] = rt
        n_ref[:] = sq_rows_to_lanes(rt)

    def stage4(g):
        s = lax.rem(g, 2)
        for q in range(2):
            c_s3(g, q).wait()
        c_z(g).wait()
        z = zown[s] + zrcv[lax.rem(g, 3)]
        ws = [rows_to_gram([stf[s, h, q, pl.ds(RD, 8)] for h in range(2)], R) for q in range(2)]
        inv = inverse_factors(ws + [z[L:]], R)
        for i in range(3):
            e_inv[g, i] = inv[i]
        for q in range(2):
            apply_keep(e_rt.at[g, q], nown.at[g, q], inv[q], stf.at[s, :, q], R)
        c_n(g).start()
        bd = block_diag(inv[2], R)
        r = times_right(z[:L], bd.T)
        d_r[g] = r
        dnown[g] = sq_lanes(r)
        for c in c_nd(g):
            c.start()

    def stage4_dense():
        kc[3]().wait()
        inv = inverse_factors([rows_to_gram([kst[h, pl.ds(RD, 8)] for h in range(2)], R)], R)
        kv_inv[:] = inv[0]
        apply_keep(kv_rt, kno, inv[0], kst, R)
        kc[4]().start()
        qc[3]().wait()
        inv = inverse_factors([rows_to_gram([qst[h, pl.ds(RD, 8)] for h in range(2)], RD)], RD)
        qo_inv[:] = inv[0]
        apply_keep(qo_rt, qno, inv[0], qst, RD)
        qc[4]().start()

    def stage5(g):
        c_n(g).wait()
        for q in range(2):
            e_n[g, q] = 1.0 / jnp.sqrt(nown[g, q] + nrcv[g, q])
        for c in c_nd(g):
            c.wait()
        d_n[g] = 1.0 / jnp.sqrt((dnown[g] + dnrcv[g, 1]) + (dnrcv[g, 0] + dnrcv[g, 2]))

    def stage5_dense():
        kc[4]().wait()
        kv_n[:] = 1.0 / jnp.sqrt(kno[:] + knr[:])
        qc[4]().wait()
        qo_n[:] = 1.0 / jnp.sqrt(qno[:] + qnr[:])

    stage1_dense()
    stage1_down(0)

    def step(t, _):
        def within(lag, stage):
            @pl.when((t >= lag) & (t < NG + lag))
            def _():
                stage(t - lag)

        def only(at, stage):
            @pl.when(t == at)
            def _():
                stage()

        @pl.when(t < NG - 1)
        def _():
            for c in loads(t + 1):
                c.start()

        @pl.when(t < NG - 2)
        def _():
            for c in loads_down(t + 2):
                c.start()

        only(2, x_load.start)
        within(0, stage2a)
        within(0, stage1)

        @pl.when(t < NG - 1)
        def _():
            stage1_down(t + 1)

        within(1, stage2b)
        within(NORM_LAG, stage5)
        only(3, stage5_dense)
        only(0, stage2_dense)
        within(1, stage2c)
        within(1, lambda g: stage3a(g, 0))
        within(2, stage3b)
        only(1, stage3b_dense)
        within(1, stage2c_down)
        within(1, lambda g: stage3a(g, 1))
        only(0, stage3a_dense)
        within(2, stage4)
        only(1, stage4_dense)
        return 0

    lax.fori_loop(0, NG + 2, step, 0)
    x_load.wait()
    for g in range(NG + 2 - NORM_LAG, NG):
        stage5(g)


def run_comm(args):
    v = pltpu.VMEM
    dma = pltpu.SemaphoreType.DMA
    out = lambda *shape: v(shape, F32)
    out_shape = [out(R, H, H), out(2, R, H, H), out(R, L, W), out(2, H, H), out(2, H, W),
                 out(NG, 3, R, L), out(NG, TWO, H, L), out(NG, TWO, L, H), out(NG, TWO, 8, L),
                 out(NG, L, L), out(NG, TWO, L, H), out(NG, 8, L),
                 out(R, L), out(H, L), out(L, H), out(8, L),
                 out(RD, L), out(H, L), out(L, W), out(8, L)]

    def pack_bufs(rows, w):
        return [v((rows, L), F32), v((rows, L), F32), v((TWO, SH, w), F32), v((SH, w), F32), v((SH, w), F32),
                v((SH, w), F32), v((TWO, SH, w), F32), v((8, L), F32), v((8, L), F32)]

    scratch = [
        v((TWO, TWO, 4, H, H), BF), v((TWO, 4, L, W), BF), v((TWO, TWO, 4, R, H), F32), v((TWO, 4, R, L), F32),
        v((TWO, H, H), BF), v((TWO, R, H), F32), v((TWO, H, W), BF), v((TWO, RD, W), F32),
        v((4, 3, H, H), BF), v((4, 3, L, W), BF), v((TWO, 3, H, H), BF), v((TWO, 3, H, W), BF),
        v((TWO, TWO, H, L), F32), v((3, 2, H, L), F32),
        v((TWO, TWO, L, H), F32), v((TWO, L, H), F32), v((TWO, L, H), F32), v((3, L, H), F32),
        v((TWO, TWO, TWO, SH, H), F32), v((TWO, TWO, SH, H), F32), v((TWO, TWO, SH, H), F32), v((3, 2, SH, H), F32),
        v((TWO, TWO, TWO, SH, H), F32),
        v((TWO, L + R, L), F32), v((3, L + R, L), F32),
        v((NG, 2, 8, L), F32), v((NG, 2, 8, L), F32), v((NG, 8, L), F32), v((NG, 3, 8, L), F32),
    ] + pack_bufs(L, H) + pack_bufs(H, W) + [
        dma((2, 9)), dma((13,)), dma((7, NG)), dma((7, NG)), dma((3, 2, NG)), dma((3, 2, NG)), dma((2, 5)), dma((2, 5)), dma((3, NG)), dma((3, NG))]
    return pl.pallas_call(
        comm_kernel,
        out_shape=out_shape,
        in_specs=[pl.BlockSpec(memory_space=pl.ANY)] * len(args),
        out_specs=[pl.BlockSpec(memory_space=pltpu.VMEM)] * len(out_shape),
        scratch_shapes=scratch,
        name="comm_kernel",
        compiler_params=pltpu.CompilerParams(collective_id=0, has_side_effects=True, vmem_limit_bytes=COMM_VMEM),
    )(*args)


def lane_copies(u, rank, slots):
    count = L // rank
    group = iota((1, L), 1) // rank
    rolled = [u] + [pltpu.roll(u, rank * s, 1) for s in range(1, count)]
    outs = []
    for m in slots:
        x = rolled[(0 - m) % count]
        for gidx in range(1, count):
            x = jnp.where(group == gidx, rolled[(gidx - m) % count], x)
        outs.append(x)
    return outs


def left_tiles(x, rank):
    a = x.astype(BF)
    r1 = x - a.astype(F32)
    b = r1.astype(BF)
    r2 = r1 - b.astype(F32)
    low = iota((1, L), 1) < RD
    if rank == R:
        return jnp.concatenate([a, jnp.where(low, r1, r2).astype(BF)], 1)
    return jnp.concatenate([a, jnp.where(low, x, r1).astype(BF), jnp.where(low, r1, r2).astype(BF)], 1)


def right_tiles(vt, rank):
    a, b, c = split3(vt)
    if rank == R:
        return jnp.concatenate([a, b, c, jnp.zeros_like(a), a, b, a, b], 0)
    return jnp.concatenate([a, b, c, a, b, a], 0)


def lanes_to_rows(n):
    return jnp.broadcast_to(n[:1], (L, L)).T


def scale_rows(vt, n):
    t = lanes_to_rows(n)
    return jnp.concatenate([vt[:, L * i:L * i + L] * t for i in range(vt.shape[1] // L)], 1)


def keep_update(p, rt, rts, rank, x_of, b_of, xo, mo, qo, step):
    copies = lane_copies(p, rank, range(TWO))
    n_cols = rt.shape[1]
    for m in range(TWO):
        rows = slice(rank * m, rank * m + rank)
        both = right_tiles(jnp.concatenate([rt[rows] * (1.0 - MOMENTUM), rts[rows] * step], 1), rank)
        out = dot(left_tiles(copies[m], rank), both)
        mo(m)[:] = b_of(m)[:] - out[:, :n_cols]
        xo(m)[:] = x_of(m)[:] - out[:, n_cols:]
        qo(m)[:] = rts[rows]


def final_kernel(ux, dx, qx, kx, vx, ox,
                 x_g, b_e, b_d, b_kv, b_qo, e_inv, e_p, e_rt, e_n, d_r, d_pt, d_n,
                 kv_inv, kv_p, kv_rt, kv_n, qo_inv, qo_p, qo_rt, qo_n,
                 gxo, gmo, gqo, uxo, umo, uqo, dxo, dmo, dqo,
                 qxo, qmo, qqo, kxo, kmo, kqo, vxo, vmo, vqo, oxo, omo, oqo,
                 x_u, x_d, load_sem, out_e, outq_e, out_d, outq_d, stack_sem,
                 p_s, rts_s, r_s, pt_s, qrow_s, xs_kv, xs_qo, mt_kv, mt_qo, qt_kv, qt_qo, isem, osem):
    i = pl.program_id(0)
    g, h = i // 2, lax.rem(i, 2)
    step = LEARN_RATE * math.sqrt(2.0)
    ins = [pltpu.make_async_copy(a, b, isem.at[k]) for k, (a, b) in enumerate(
        [(kx, xs_kv.at[0]), (vx, xs_kv.at[1]), (qx, xs_qo.at[0]), (ox, xs_qo.at[1])])]
    outs = [pltpu.make_async_copy(b, a, osem.at[k]) for k, (a, b) in enumerate(
        [(kxo, xs_kv.at[0]), (vxo, xs_kv.at[1]), (qxo, xs_qo.at[0]), (oxo, xs_qo.at[1]),
         (kmo, mt_kv.at[0]), (vmo, mt_kv.at[1]), (qmo, mt_qo.at[0]), (omo, mt_qo.at[1]),
         (kqo, qt_kv.at[0]), (vqo, qt_kv.at[1]), (qqo, qt_qo.at[0]), (oqo, qt_qo.at[1])])]

    def stack_outs(j):
        s = lax.rem(j, OUT_SLOTS)
        e = pl.ds(2 * j, 2)
        pairs = [(out_e.at[s, 0, 0], gxo), (out_e.at[s, 0, 1], gmo), (outq_e.at[s, 0], gqo),
                 (out_e.at[s, 1, 0], uxo), (out_e.at[s, 1, 1], umo), (outq_e.at[s, 1], uqo),
                 (out_d.at[s, 0], dxo), (out_d.at[s, 1], dmo), (outq_d.at[s], dqo)]
        return [pltpu.make_async_copy(a, b.at[e], stack_sem.at[k, s]) for k, (a, b) in enumerate(pairs)]

    def stack_ins(j):
        s = lax.rem(j, IN_SLOTS)
        e = pl.ds(2 * j, 2)
        return [pltpu.make_async_copy(a.at[e], b.at[s], load_sem.at[k, s]) for k, (a, b) in enumerate(((ux, x_u), (dx, x_d)))]

    slot, ins_slot = lax.rem(i, OUT_SLOTS), lax.rem(i, IN_SLOTS)

    @pl.when(i == 0)
    def _():
        for j in range(IN_SLOTS):
            for c in stack_ins(j):
                c.start()
        for c in ins:
            c.start()

    for c in stack_ins(i):
        c.wait()

    @pl.when(i >= OUT_SLOTS)
    def _():
        for c in stack_outs(i - OUT_SLOTS):
            c.wait()

    @pl.when(h == 0)
    def _():
        for q in range(TWO):
            p_s[q] = times_right(e_p[g, q], block_diag(e_inv[g, q], R).T)
            rts_s[q] = scale_rows(e_rt[g, q], e_n[g, q])
        pt_s[:] = times_left(block_diag(e_inv[g, 2], R), jnp.concatenate([d_pt[g, 0], d_pt[g, 1]], 1))
        r_s[0] = d_r[g] * (1.0 - MOMENTUM)
        qpack = d_r[g] * d_n[g][:1]
        r_s[1] = qpack * step
        qrow_s[:] = qpack.T

    @pl.when(h == 1)
    def _():
        for q in range(TWO):
            p_s[q] = pltpu.roll(p_s[q], RD, 1)
            r_s[q] = pltpu.roll(r_s[q], RD, 1)

    half = pl.ds(h * RD, RD)
    for q, x in enumerate((lambda m: x_g.at[i * 2 + m], lambda m: x_u.at[ins_slot, m])):
        keep_update(p_s[q], e_rt[g, q, half], rts_s[q, half], R, x, lambda m: b_e.at[q, i * 2 + m],
                    lambda m: out_e.at[slot, q, 0, m], lambda m: out_e.at[slot, q, 1, m],
                    lambda m: outq_e.at[slot, q, m], step)
    rcopies = lane_copies(r_s[0], R, range(TWO))
    qcopies = lane_copies(r_s[1], R, range(TWO))
    pt, qrows = pt_s[half], qrow_s[half]
    for m in range(TWO):
        rows = slice(R * m, R * m + R)
        out = dot(jnp.concatenate([left_tiles(rcopies[m], R), left_tiles(qcopies[m], R)], 0), right_tiles(pt[rows], R))
        out_d[slot, 1, m] = b_d[i * 2 + m] - out[:L]
        out_d[slot, 0, m] = x_d[ins_slot, m] - out[L:]
        outq_d[slot, m] = qrows[rows]
    for c in stack_outs(i):
        c.start()

    @pl.when(i < 2 * NG - IN_SLOTS)
    def _():
        for c in stack_ins(i + IN_SLOTS):
            c.start()

    @pl.when(i == 1)
    def _():
        for c in ins:
            c.wait()
        for p0, inv, rt, n, rank, xs, b, mt, qt, size in (
                (kv_p, kv_inv, kv_rt, kv_n, R, xs_kv, b_kv, mt_kv, qt_kv, step),
                (qo_p, qo_inv, qo_rt, qo_n, RD, xs_qo, b_qo, mt_qo, qt_qo, LEARN_RATE)):
            keep_update(times_right(p0[:], block_diag(inv[:], rank).T), rt[:], scale_rows(rt[:], n[:]), rank,
                        xs.at.__getitem__, b.at.__getitem__,
                        xs.at.__getitem__, mt.at.__getitem__, qt.at.__getitem__, size)
        for c in outs:
            c.start()

    @pl.when(i == 2 * NG - 1)
    def _():
        for c in outs:
            c.wait()
        for k in range(OUT_SLOTS):
            for c in stack_outs(i - k):
                c.wait()


def run_final(xs, packs):
    hbm = pl.BlockSpec(memory_space=pl.ANY)
    v = pltpu.VMEM

    out = lambda *shape: jax.ShapeDtypeStruct(shape, F32)
    big = [out(R, H, H), out(R, H, H), out(R, R, H)]
    stacks = big + big + [out(R, L, W), out(R, L, W), out(R, R, L)]
    wide = [out(H, W), out(H, W), out(RD, W)]
    narrow = [out(H, H), out(H, H), out(R, H)]
    return pl.pallas_call(
        final_kernel,
        grid=(2 * NG,),
        out_shape=stacks + wide + narrow + narrow + wide,
        in_specs=[hbm] * len(xs) + [pl.BlockSpec(memory_space=v)] * len(packs),
        out_specs=[hbm] * len(stacks + wide + narrow + narrow + wide),
        scratch_shapes=[v((IN_SLOTS, TWO, H, H), F32), v((IN_SLOTS, TWO, L, W), F32),
                        pltpu.SemaphoreType.DMA((TWO, IN_SLOTS)), v((OUT_SLOTS, TWO, TWO, TWO, H, H), F32), v((OUT_SLOTS, TWO, TWO, R, H), F32),
                        v((OUT_SLOTS, TWO, TWO, L, W), F32), v((OUT_SLOTS, 2, R, L), F32),
                        pltpu.SemaphoreType.DMA((len(stacks), OUT_SLOTS)),
                        v((TWO, H, L), F32), v((TWO, L, H), F32), v((TWO, L, L), F32), v((L, W), F32), v((L, L), F32),
                        v((TWO, H, H), F32), v((TWO, H, W), F32), v((TWO, H, H), F32), v((TWO, H, W), F32),
                        v((TWO, R, H), F32), v((TWO, RD, W), F32),
                        pltpu.SemaphoreType.DMA((4,)), pltpu.SemaphoreType.DMA((12,))],
        name="final_kernel",
        compiler_params=pltpu.CompilerParams(vmem_limit_bytes=FINAL_VMEM, dimension_semantics=("arbitrary",)),
    )(*xs, *packs)


def solution(mesh):
    dense_w = P(('layer', 'fsdp'), 'tp')
    dense_f = P(('layer', 'tp'), None)
    stack_w = P('layer', 'fsdp', 'tp')
    stack_f = P('layer', 'tp', None)
    down_f = P('layer', 'fsdp', None)
    in_specs = (dense_w, dense_w, dense_w, dense_f) * 4 + (stack_w, stack_w, stack_w, stack_f) * 2 + (stack_w, stack_w, stack_w, down_f)
    out_specs = (dense_w, dense_w, dense_f) * 4 + (stack_w, stack_w, stack_f) * 2 + (stack_w, stack_w, down_f)

    def local_step(*b):
        x, m, g = b[0::4], b[1::4], b[2::4]
        q = [jnp.swapaxes(f, -1, -2) for f in b[3::4]]
        comm_in = []
        for i in (4, 5, 6, 0, 1, 2, 3):
            comm_in += [m[i], g[i], q[i]]
        comm_in.append(x[4])
        packs = [pltpu.with_memory_space_constraint(a, pltpu.VMEM) for a in run_comm(comm_in)]
        outs = run_final([x[i] for i in (5, 6, 0, 1, 2, 3)], packs)
        outs = list(outs[9:]) + list(outs[:9])
        for i in range(2, 21, 3):
            outs[i] = jnp.swapaxes(outs[i], -1, -2)
        return tuple(outs)

    return jax.shard_map(local_step, mesh=mesh, in_specs=in_specs, out_specs=out_specs, check_vma=False)
```

```python
import math
import jax
import jax.numpy as jnp
from jax import lax
from jax.experimental import pallas as pl
from jax.experimental.pallas import tpu as pltpu
from jax.sharding import PartitionSpec as P


MOMENTUM = 0.9
LEARN_RATE = 0.3
F32 = jnp.float32
BF = jnp.bfloat16
MESH = pl.DeviceIdType.MESH
NG = 8
PACK = 4
L = 128
H = 256
W = 512
R = 32
RD = 64
COMM_VMEM = 22 << 20
FINAL_VMEM = 22 << 20
NORM_LAG = 4
OUT_SLOTS = 3
IN_SLOTS = 5
TWO = 2
HR = R // 2
SH = 72


def dot(a, b):
    return jnp.dot(a, b, preferred_element_type=F32)


def split3(x):
    a = x.astype(BF)
    r = x - a.astype(F32)
    b = r.astype(BF)
    c = (r - b.astype(F32)).astype(BF)
    return a, b, c


def iota(shape, axis):
    return lax.broadcasted_iota(jnp.int32, shape, axis)


def row_factor(pieces, count, v, rank):
    v1, v2, v3 = split3(v)
    group = iota((1, L), 1) // rank
    acc = acc2 = None
    for m in range(count):
        b12, b1, b3 = pieces(m)
        mask = jnp.where(group == m, 1.0, 0.0).astype(BF)
        w1, w2, w3 = v1 * mask, v2 * mask, v3 * mask
        t = dot(b12, jnp.concatenate([w1, w2], 1))
        u = dot(b1, w3) + dot(b3, w1)
        acc = t if acc is None else acc + t
        acc2 = u if acc2 is None else acc2 + u
    n = acc2.shape[0]
    return acc[:n, :L] + acc2 + (acc[:n, L:] + acc[n:, :L]) + acc[n:, L:]


def col_factor(ut, b1, b2, b3, m, rank):
    lhs = jnp.concatenate([t[rank * m:rank * m + rank] for t in ut], 0)
    o1 = dot(lhs, b1)
    o2 = dot(lhs[:2 * rank], b2)
    o3 = dot(lhs[:rank], b3)
    return o1[:rank] + (o1[rank:2 * rank] + o2[:rank]) + (o1[2 * rank:] + o2[rank:] + o3)


def gram(ut, u, rank):
    full = dot(jnp.concatenate([ut[0], ut[1]], 0), jnp.concatenate([u[0], u[1]], 1))
    low = dot(ut[2], u[0]) + dot(ut[0], u[2])
    g = full[:L, :L] + (full[:L, L:] + full[L:, :L] + low) + full[L:, L:]
    group = iota((rank, L), 1) // rank
    out = jnp.where(group == 0, g[:rank], 0.0)
    for m in range(1, L // rank):
        out = out + jnp.where(group == m, g[rank * m:rank * m + rank], 0.0)
    return out


def inverse_factors(grams, rank):
    lane = iota((rank, L), 1)
    row = iota((rank, L), 0)
    base = (lane // rank) * rank
    col = lane - base
    mats = list(grams)
    for k0 in range(0, rank, 16):
        cols = [[jnp.take_along_axis(a, base + (k0 + j), axis=1) for j in range(16)] for a in mats]
        for j in range(16):
            k = k0 + j
            below = row > k
            for i, a in enumerate(mats):
                ck = cols[i][j]
                factor = jnp.where(below, ck * (1.0 / ck[k:k + 1]), 0.0)
                pivot = jnp.where(col[:1] == k, 1.0, a[k:k + 1])
                mats[i] = jnp.where(below & (col == k), 0.0, a) - factor * pivot
                for l in range(j + 1, 16):
                    cl = cols[i][l]
                    cols[i][l] = cl - factor * cl[k:k + 1]
    out = []
    for a in mats:
        diag = jnp.take_along_axis(a, base + row, axis=1)
        unit = jnp.where(col < row, a, jnp.where(col == row, 1.0, 0.0))
        out.append(unit * (1.0 / jnp.sqrt(diag)))
    return out


def block_diag(inv, rank):
    group = iota((rank, L), 1) // rank
    return jnp.concatenate([jnp.where(group == m, inv, 0.0) for m in range(L // rank)], 0)


def times_right(u, t):
    u1, u2, u3 = split3(u)
    t1, t2, t3 = split3(t)
    t12 = jnp.concatenate([t1, t2], 1)
    a = dot(jnp.concatenate([u1, u2], 1), jnp.concatenate([t12, t12], 0))
    b = dot(jnp.concatenate([u1, u3], 1), jnp.concatenate([t3, t1], 0))
    return a[:, :L] + (a[:, L:] + b)


def times_left(b, v):
    b1, b2, b3 = split3(b)
    v1, v2, v3 = split3(v)
    b12 = jnp.concatenate([b1, b2], 1)
    hi = dot(b12, jnp.concatenate([v1, v1], 0))
    lo = dot(b12, jnp.concatenate([v2, v2], 0))
    lo = lo + dot(jnp.concatenate([b1, b3], 1), jnp.concatenate([v3, v1], 0))
    return hi + lo


def sq_rows_to_lanes(v):
    s = v * v
    f = s[:, :L]
    for i in range(1, v.shape[1] // L):
        f = f + s[:, L * i:L * i + L]
    return jnp.broadcast_to(jnp.sum(f.T, 0, keepdims=True), (8, L))


def sq_lanes(u):
    return jnp.broadcast_to(jnp.sum(u * u, 0, keepdims=True), (8, L))


def gram_to_rows(w, half, rank):
    h = rank // 2
    return jnp.concatenate([w[half * h + 8 * i:half * h + 8 * i + 8] for i in range(h // 8)], 1)


def rows_to_gram(halves, rank):
    parts = []
    for x in halves:
        parts.extend([x[:, L * i:L * i + L] for i in range(rank // 16)])
    return jnp.concatenate(parts, 0)


def comm_kernel(gm, gg, gq, um, ug, uq, dm, dg, dq,
                wqm, wqg, wqf, wkm, wkg, wkf, wvm, wvg, wvf, wom, wog, wof, gx,
                x_g, b_e, b_d, b_kv, b_qo, e_inv, e_p, e_rt, e_n, d_r, d_pt, d_n,
                kv_inv, kv_p, kv_rt, kv_n, qo_inv, qo_p, qo_rt, qo_n,
                gs_e, gs_d, qs_e, qs_d, gs_kv, qs_kv, gs_qo, qs_qo,
                z_e, z_d, z_kv, z_qo,
                pown, prcv, down, drc1, dxs, dxr, sown, src1, sxs, sxr, stf, zown, zrcv, zw, zt,
                nown, nrcv, dnown, dnrcv,
                kpo, kpr, kso, ksr, kxs, kxr, kst, kno, knr,
                qpo, qpr, qso, qsr, qxs, qxr, qst, qno, qnr,
                lsem, dsem, send, recv, sends, recvs, sendk, recvk, sendn, recvn):
    tp = lax.axis_index("tp")
    fs = lax.axis_index("fsdp")
    core = lax.rem(fs, 2)
    ypeer = {"tp": 1 - tp}
    sib = {"fsdp": fs + 1 - 2 * core}
    xpeer = {"fsdp": lax.rem(fs + 2, 4)}

    def loads(g):
        s = lax.rem(g, 2)
        e = pl.ds(g * PACK, PACK)
        pairs = [(gm.at[e], b_e.at[0, e]), (gg.at[e], gs_e.at[s, 0]), (gq.at[e], qs_e.at[s, 0]),
                 (um.at[e], b_e.at[1, e]), (ug.at[e], gs_e.at[s, 1]), (uq.at[e], qs_e.at[s, 1])]
        return [pltpu.make_async_copy(a, b, lsem.at[s, i]) for i, (a, b) in enumerate(pairs)]

    def loads_down(g):
        s = lax.rem(g, 2)
        e = pl.ds(g * PACK, PACK)
        pairs = [(dm.at[e], b_d.at[e]), (dg.at[e], gs_d.at[s]), (dq.at[e], qs_d.at[s])]
        return [pltpu.make_async_copy(a, b, lsem.at[s, len(pairs) * 2 + i]) for i, (a, b) in enumerate(pairs)]

    dense_loads = [pltpu.make_async_copy(a, b, dsem.at[i]) for i, (a, b) in enumerate([
        (wkm, b_kv.at[0]), (wkg, gs_kv.at[0]), (wkf, qs_kv.at[0]),
        (wvm, b_kv.at[1]), (wvg, gs_kv.at[1]), (wvf, qs_kv.at[1]),
        (wqm, b_qo.at[0]), (wqg, gs_qo.at[0]), (wqf, qs_qo.at[0]),
        (wom, b_qo.at[1]), (wog, gs_qo.at[1]), (wof, qs_qo.at[1])])]
    x_load = pltpu.make_async_copy(gx, x_g, dsem.at[len(dense_loads)])
    for c in dense_loads:
        c.start()

    barrier = pltpu.get_barrier_semaphore()
    fours = [{"fsdp": lax.rem(fs + i, 4)} for i in (1, 2, 3)]
    for dev in [ypeer] + fours:
        pl.semaphore_signal(barrier, inc=1, device_id=dev, device_id_type=MESH)
    pl.semaphore_wait(barrier, 4)

    def remote(src, dst, ss, rs, dev):
        return pltpu.make_async_remote_copy(src_ref=src, dst_ref=dst, send_sem=ss, recv_sem=rs,
                                            device_id=dev, device_id_type=MESH)

    def c_p(g, q):
        return remote(pown.at[lax.rem(g, 2), q], prcv.at[lax.rem(g, 3), q], send.at[q, g], recv.at[q, g], ypeer)

    def c_d1(g):
        return remote(down.at[lax.rem(g, 2), 1 - core], drc1.at[lax.rem(g, 2)], send.at[2, g], recv.at[2, g], sib)

    def c_d2(g):
        return remote(dxs.at[lax.rem(g, 2)], dxr.at[lax.rem(g, 3)], send.at[3, g], recv.at[3, g], xpeer)

    def c_d3(g):
        return remote(d_pt.at[g, core], d_pt.at[g, core], send.at[4, g], recv.at[4, g], sib)

    def c_s1(g, q):
        return remote(sown.at[lax.rem(g, 2), 1 - core, q], src1.at[lax.rem(g, 2), q], sends.at[0, q, g], recvs.at[0, q, g], sib)

    def c_s2(g, q):
        return remote(sxs.at[lax.rem(g, 2), q], sxr.at[lax.rem(g, 3), q], sends.at[1, q, g], recvs.at[1, q, g], xpeer)

    def c_s3(g, q):
        return remote(stf.at[lax.rem(g, 2), core, q], stf.at[lax.rem(g, 2), core, q], sends.at[2, q, g], recvs.at[2, q, g], sib)

    def c_z(g):
        return remote(zown.at[lax.rem(g, 2)], zrcv.at[lax.rem(g, 3)], send.at[5, g], recv.at[5, g], ypeer)

    def c_w(g):
        s = lax.rem(g, 2)
        return remote(zt.at[s, core], zt.at[s, core], send.at[7, g], recv.at[7, g], sib)

    def c_n(g):
        return remote(nown.at[g], nrcv.at[g], send.at[6, g], recv.at[6, g], ypeer)

    def c_nd(g):
        return [remote(dnown.at[g], dnrcv.at[g, i], sendn.at[i, g], recvn.at[i, g], fours[i]) for i in range(3)]

    def dense_copies(i, po, pr, so, sr, xs, xr, st, no, nr):
        k = lambda j: (sendk.at[i, j], recvk.at[i, j])
        return (lambda: remote(po, pr, *k(0), ypeer),
                lambda: remote(so.at[1 - core], sr, *k(1), sib),
                lambda: remote(xs, xr, *k(2), xpeer),
                lambda: remote(st.at[core], st.at[core], *k(3), sib),
                lambda: remote(no, nr, *k(4), ypeer))

    kc = dense_copies(0, kpo, kpr, kso, ksr, kxs, kxr, kst, kno, knr)
    qc = dense_copies(1, qpo, qpr, qso, qsr, qxs, qxr, qst, qno, qnr)

    def terms(b_ref, g_ref, z_ref):
        for r0 in range(0, b_ref.shape[0], RD):
            rs = pl.ds(r0, RD)
            b = b_ref[rs]
            if g_ref is not None:
                b = b + g_ref[rs].astype(F32)
                b_ref[rs] = b
            b1, b2, b3 = split3(b)
            z_ref[0, rs] = b1
            z_ref[1, rs] = b2
            z_ref[2, rs] = b3

    def pieces_of(z_ref):
        n, w = z_ref.shape[1:]
        return z_ref[0:2].reshape(2 * n, w), z_ref[0], z_ref[2]

    def stage1(g):
        s = lax.rem(g, 2)
        for c in loads(g):
            c.wait()

        def one(q, _):
            for m in range(PACK):
                terms(b_e.at[q, g * PACK + m], gs_e.at[s, q, m], z_e.at[m])
            v = qs_e[s, q].reshape(L, H).T
            pown[s, q] = row_factor(lambda m: pieces_of(z_e.at[m]), PACK, v, R)
            c_p(g, q).start()
            return 0

        lax.fori_loop(0, 2, one, 0)

    def stage1_down(g):
        s = lax.rem(g, 2)
        for c in loads_down(g):
            c.wait()
        ut = split3(qs_d[s].reshape(L, L))
        for m in range(PACK):
            terms(b_d.at[g * PACK + m], gs_d.at[s, m], z_d.at[m])
            part = col_factor(ut, z_d[m, 0], z_d[m, 1], z_d[m, 2], m, R)
            down[s, 0, pl.ds(R * m, R)] = part[:, :H]
            down[s, 1, pl.ds(R * m, R)] = part[:, H:]
        c_d1(g).start()

    low = iota((1, L), 1) < RD

    def stage1_dense():
        for c in dense_loads[:6]:
            c.wait()
        for i in range(2):
            terms(b_kv.at[i], gs_kv.at[i], z_kv.at[i])
        v = jnp.concatenate([qs_kv[0], qs_kv[1], qs_kv[0], qs_kv[1]], 0).T
        u = row_factor(lambda m: pieces_of(z_kv.at[m % 2]), 4, v, R)
        kpo[:] = jnp.where(low, u[:L], u[L:])
        kc[0]().start()
        for c in dense_loads[6:]:
            c.wait()
        for c in loads_down(0) + loads(0) + loads_down(1):
            c.start()
        for i in range(2):
            terms(b_qo.at[i], gs_qo.at[i], z_qo.at[i])
        v = qs_qo[:].reshape(L, W).T
        qpo[:] = row_factor(lambda m: pieces_of(z_qo.at[m]), 2, v, RD)
        qc[0]().start()

    def stage2a(g):
        s = lax.rem(g, 2)
        c_d1(g).wait()
        dxs[s] = down[s, core] + drc1[s]
        c_d2(g).start()

    def stage2b(g):
        c_d2(g).wait()
        d_pt[g, core] = dxs[lax.rem(g, 2)] + dxr[lax.rem(g, 3)]
        c_d3(g).start()

    def s_and_gram(u, rank, count, z_of, so):
        ut = u.T
        up, utp = split3(u), split3(ut)
        half = L // rank // 2
        for m in range(count):
            z = z_of(m)
            so[m // half, pl.ds(rank * (m % half), rank)] = col_factor(utp, z[0], z[1], z[2], m, rank)
        w = gram(utp, up, rank)
        for h in range(2):
            so[h, pl.ds(RD, 8)] = gram_to_rows(w, h, rank)

    def stage2c(g):
        s = lax.rem(g, 2)

        def one(q, _):
            c_p(g, q).wait()
            u = pown[s, q] + prcv[lax.rem(g, 3), q]
            e_p[g, q] = u
            for m in range(PACK):
                terms(b_e.at[q, g * PACK + m], None, z_e.at[m])
            s_and_gram(u, R, PACK, z_e.at.__getitem__, sown.at[s, :, q])
            c_s1(g, q).start()
            return 0

        lax.fori_loop(0, 2, one, 0)

    def stage2c_down(g):
        s = lax.rem(g, 2)
        for m in range(PACK):
            terms(b_d.at[g * PACK + m], None, z_d.at[m])
        c_d3(g).wait()
        vt = jnp.concatenate([d_pt[g, 0], d_pt[g, 1]], 1)
        v = vt.T
        zown[s, pl.ds(0, L)] = row_factor(lambda m: pieces_of(z_d.at[m]), PACK, v, R)
        w = gram(split3(vt), split3(v), R)
        zw[0] = w[:HR]
        zw[1] = w[HR:]
        zown[s, pl.ds(L, HR)] = zw[core]
        c_z(g).start()

    def stage3w(g):
        s = lax.rem(g, 2)
        c_z(g).wait()
        zt[s, core] = zown[s, pl.ds(L, HR)] + zrcv[lax.rem(g, 3), pl.ds(L, HR)]
        c_w(g).start()

    def stage2_dense():
        kc[0]().wait()
        u = kpo[:] + kpr[:]
        t = pltpu.roll(u, RD, 1)
        u = jnp.concatenate([jnp.where(low, u, t), jnp.where(low, t, u)], 0)
        kv_p[:] = u
        s_and_gram(u, R, 4, lambda m: z_kv.at[m % 2], kso)
        kc[1]().start()
        qc[0]().wait()
        u = qpo[:] + qpr[:]
        qo_p[:] = u
        s_and_gram(u, RD, 2, lambda m: z_qo.at[m], qso)
        qc[1]().start()

    def stage3a(g, q):
        s = lax.rem(g, 2)
        c_s1(g, q).wait()
        sxs[s, q] = sown[s, core, q] + src1[s, q]
        c_s2(g, q).start()

    def stage3b(g):
        for q in range(2):
            c_s2(g, q).wait()
            stf[lax.rem(g, 2), core, q] = sxs[lax.rem(g, 2), q] + sxr[lax.rem(g, 3), q]
            c_s3(g, q).start()

    def stage3a_dense():
        for cs, so, sr, xs in ((kc, kso, ksr, kxs), (qc, qso, qsr, qxs)):
            cs[1]().wait()
            xs[:] = so[core] + sr[:]
            cs[2]().start()

    def stage3b_dense():
        for cs, xs, xr, st in ((kc, kxs, kxr, kst), (qc, qxs, qxr, qst)):
            cs[2]().wait()
            st[core] = xs[:] + xr[:]
            cs[3]().start()

    def apply_keep(rt_ref, n_ref, inv, st, rank):
        bd = block_diag(inv, rank)
        vt = jnp.concatenate([st[0, pl.ds(0, RD)], st[1, pl.ds(0, RD)]], 0)
        rt = times_left(bd, vt)
        rt_ref[:] = rt
        n_ref[:] = sq_rows_to_lanes(rt)

    def stage4(g):
        s = lax.rem(g, 2)
        for q in range(2):
            c_s3(g, q).wait()
        c_w(g).wait()
        z = zown[s, pl.ds(0, L)] + zrcv[lax.rem(g, 3), pl.ds(0, L)]
        ws = [rows_to_gram([stf[s, h, q, pl.ds(RD, 8)] for h in range(2)], R) for q in range(2)]
        inv = inverse_factors(ws + [jnp.concatenate([zt[s, 0], zt[s, 1]], 0)], R)
        for i in range(3):
            e_inv[g, i] = inv[i]
        for q in range(2):
            apply_keep(e_rt.at[g, q], nown.at[g, q], inv[q], stf.at[s, :, q], R)
        c_n(g).start()
        bd = block_diag(inv[2], R)
        r = times_right(z, bd.T)
        d_r[g] = r
        dnown[g] = sq_lanes(r)
        for c in c_nd(g):
            c.start()

    def stage4_dense():
        kc[3]().wait()
        inv = inverse_factors([rows_to_gram([kst[h, pl.ds(RD, 8)] for h in range(2)], R)], R)
        kv_inv[:] = inv[0]
        apply_keep(kv_rt, kno, inv[0], kst, R)
        kc[4]().start()
        qc[3]().wait()
        inv = inverse_factors([rows_to_gram([qst[h, pl.ds(RD, 8)] for h in range(2)], RD)], RD)
        qo_inv[:] = inv[0]
        apply_keep(qo_rt, qno, inv[0], qst, RD)
        qc[4]().start()

    def stage5(g):
        c_n(g).wait()
        for q in range(2):
            e_n[g, q] = 1.0 / jnp.sqrt(nown[g, q] + nrcv[g, q])
        for c in c_nd(g):
            c.wait()
        d_n[g] = 1.0 / jnp.sqrt((dnown[g] + dnrcv[g, 1]) + (dnrcv[g, 0] + dnrcv[g, 2]))

    def stage5_dense():
        kc[4]().wait()
        kv_n[:] = 1.0 / jnp.sqrt(kno[:] + knr[:])
        qc[4]().wait()
        qo_n[:] = 1.0 / jnp.sqrt(qno[:] + qnr[:])

    stage1_dense()
    stage1_down(0)

    def step(t, _):
        def within(lag, stage):
            @pl.when((t >= lag) & (t < NG + lag))
            def _():
                stage(t - lag)

        def only(at, stage):
            @pl.when(t == at)
            def _():
                stage()

        @pl.when(t < NG - 1)
        def _():
            for c in loads(t + 1):
                c.start()

        @pl.when(t < NG - 2)
        def _():
            for c in loads_down(t + 2):
                c.start()

        only(2, x_load.start)
        within(0, stage2a)
        within(0, stage1)

        @pl.when(t < NG - 1)
        def _():
            stage1_down(t + 1)

        within(1, stage2b)
        within(NORM_LAG, stage5)
        only(3, stage5_dense)
        only(0, stage2_dense)
        within(1, stage2c)
        within(1, lambda g: stage3a(g, 0))
        within(2, stage3b)
        only(1, stage3b_dense)
        within(2, stage3w)
        within(1, stage2c_down)
        within(1, lambda g: stage3a(g, 1))
        only(0, stage3a_dense)
        within(2, stage4)
        only(1, stage4_dense)
        return 0

    lax.fori_loop(0, NG + 2, step, 0)
    x_load.wait()
    for g in range(NG + 2 - NORM_LAG, NG):
        stage5(g)


def run_comm(args):
    v = pltpu.VMEM
    dma = pltpu.SemaphoreType.DMA
    out = lambda *shape: v(shape, F32)
    out_shape = [out(R, H, H), out(2, R, H, H), out(R, L, W), out(2, H, H), out(2, H, W),
                 out(NG, 3, R, L), out(NG, TWO, H, L), out(NG, TWO, L, H), out(NG, TWO, 8, L),
                 out(NG, L, L), out(NG, TWO, L, H), out(NG, 8, L),
                 out(R, L), out(H, L), out(L, H), out(8, L),
                 out(RD, L), out(H, L), out(L, W), out(8, L)]

    def pack_bufs(rows, w):
        return [v((rows, L), F32), v((rows, L), F32), v((TWO, SH, w), F32), v((SH, w), F32), v((SH, w), F32),
                v((SH, w), F32), v((TWO, SH, w), F32), v((8, L), F32), v((8, L), F32)]

    scratch = [
        v((TWO, TWO, 4, H, H), BF), v((TWO, 4, L, W), BF), v((TWO, TWO, 4, R, H), F32), v((TWO, 4, R, L), F32),
        v((TWO, H, H), BF), v((TWO, R, H), F32), v((TWO, H, W), BF), v((TWO, RD, W), F32),
        v((4, 3, H, H), BF), v((4, 3, L, W), BF), v((TWO, 3, H, H), BF), v((TWO, 3, H, W), BF),
        v((TWO, TWO, H, L), F32), v((3, 2, H, L), F32),
        v((TWO, TWO, L, H), F32), v((TWO, L, H), F32), v((TWO, L, H), F32), v((3, L, H), F32),
        v((TWO, TWO, TWO, SH, H), F32), v((TWO, TWO, SH, H), F32), v((TWO, TWO, SH, H), F32), v((3, 2, SH, H), F32),
        v((TWO, TWO, TWO, SH, H), F32),
        v((TWO, L + HR, L), F32), v((3, L + HR, L), F32), v((TWO, HR, L), F32), v((TWO, TWO, HR, L), F32),
        v((NG, 2, 8, L), F32), v((NG, 2, 8, L), F32), v((NG, 8, L), F32), v((NG, 3, 8, L), F32),
    ] + pack_bufs(L, H) + pack_bufs(H, W) + [
        dma((2, 9)), dma((13,)), dma((8, NG)), dma((8, NG)), dma((3, 2, NG)), dma((3, 2, NG)), dma((2, 5)), dma((2, 5)), dma((3, NG)), dma((3, NG))]
    return pl.pallas_call(
        comm_kernel,
        out_shape=out_shape,
        in_specs=[pl.BlockSpec(memory_space=pl.ANY)] * len(args),
        out_specs=[pl.BlockSpec(memory_space=pltpu.VMEM)] * len(out_shape),
        scratch_shapes=scratch,
        name="comm_kernel",
        compiler_params=pltpu.CompilerParams(collective_id=0, has_side_effects=True, vmem_limit_bytes=COMM_VMEM),
    )(*args)


def lane_copies(u, rank, slots):
    count = L // rank
    group = iota((1, L), 1) // rank
    rolled = [u] + [pltpu.roll(u, rank * s, 1) for s in range(1, count)]
    outs = []
    for m in slots:
        x = rolled[(0 - m) % count]
        for gidx in range(1, count):
            x = jnp.where(group == gidx, rolled[(gidx - m) % count], x)
        outs.append(x)
    return outs


def left_tiles(x, rank):
    a = x.astype(BF)
    r1 = x - a.astype(F32)
    b = r1.astype(BF)
    r2 = r1 - b.astype(F32)
    low = iota((1, L), 1) < RD
    if rank == R:
        return jnp.concatenate([a, jnp.where(low, r1, r2).astype(BF)], 1)
    return jnp.concatenate([a, jnp.where(low, x, r1).astype(BF), jnp.where(low, r1, r2).astype(BF)], 1)


def right_tiles(vt, rank):
    a, b, c = split3(vt)
    if rank == R:
        return jnp.concatenate([a, b, c, jnp.zeros_like(a), a, b, a, b], 0)
    return jnp.concatenate([a, b, c, a, b, a], 0)


def lanes_to_rows(n):
    return jnp.broadcast_to(n[:1], (L, L)).T


def scale_rows(vt, n):
    t = lanes_to_rows(n)
    return jnp.concatenate([vt[:, L * i:L * i + L] * t for i in range(vt.shape[1] // L)], 1)


def keep_update(p, rt, rts, rank, x_of, b_of, xo, mo, qo, step):
    copies = lane_copies(p, rank, range(TWO))
    n_cols = rt.shape[1]
    for m in range(TWO):
        rows = slice(rank * m, rank * m + rank)
        both = right_tiles(jnp.concatenate([rt[rows] * (1.0 - MOMENTUM), rts[rows] * step], 1), rank)
        out = dot(left_tiles(copies[m], rank), both)
        mo(m)[:] = b_of(m)[:] - out[:, :n_cols]
        xo(m)[:] = x_of(m)[:] - out[:, n_cols:]
        qo(m)[:] = rts[rows]


def final_kernel(ux, dx, qx, kx, vx, ox,
                 x_g, b_e, b_d, b_kv, b_qo, e_inv, e_p, e_rt, e_n, d_r, d_pt, d_n,
                 kv_inv, kv_p, kv_rt, kv_n, qo_inv, qo_p, qo_rt, qo_n,
                 gxo, gmo, gqo, uxo, umo, uqo, dxo, dmo, dqo,
                 qxo, qmo, qqo, kxo, kmo, kqo, vxo, vmo, vqo, oxo, omo, oqo,
                 x_u, x_d, load_sem, out_e, outq_e, out_d, outq_d, stack_sem,
                 p_s, rts_s, r_s, pt_s, qrow_s, xs_kv, xs_qo, mt_kv, mt_qo, qt_kv, qt_qo, isem, osem):
    i = pl.program_id(0)
    g, h = i // 2, lax.rem(i, 2)
    step = LEARN_RATE * math.sqrt(2.0)
    ins = [pltpu.make_async_copy(a, b, isem.at[k]) for k, (a, b) in enumerate(
        [(kx, xs_kv.at[0]), (vx, xs_kv.at[1]), (qx, xs_qo.at[0]), (ox, xs_qo.at[1])])]
    outs = [pltpu.make_async_copy(b, a, osem.at[k]) for k, (a, b) in enumerate(
        [(kxo, xs_kv.at[0]), (vxo, xs_kv.at[1]), (qxo, xs_qo.at[0]), (oxo, xs_qo.at[1]),
         (kmo, mt_kv.at[0]), (vmo, mt_kv.at[1]), (qmo, mt_qo.at[0]), (omo, mt_qo.at[1]),
         (kqo, qt_kv.at[0]), (vqo, qt_kv.at[1]), (qqo, qt_qo.at[0]), (oqo, qt_qo.at[1])])]

    def stack_outs(j):
        s = lax.rem(j, OUT_SLOTS)
        e = pl.ds(2 * j, 2)
        pairs = [(out_e.at[s, 0, 0], gxo), (out_e.at[s, 0, 1], gmo), (outq_e.at[s, 0], gqo),
                 (out_e.at[s, 1, 0], uxo), (out_e.at[s, 1, 1], umo), (outq_e.at[s, 1], uqo),
                 (out_d.at[s, 0], dxo), (out_d.at[s, 1], dmo), (outq_d.at[s], dqo)]
        return [pltpu.make_async_copy(a, b.at[e], stack_sem.at[k, s]) for k, (a, b) in enumerate(pairs)]

    def stack_ins(j):
        s = lax.rem(j, IN_SLOTS)
        e = pl.ds(2 * j, 2)
        return [pltpu.make_async_copy(a.at[e], b.at[s], load_sem.at[k, s]) for k, (a, b) in enumerate(((ux, x_u), (dx, x_d)))]

    slot, ins_slot = lax.rem(i, OUT_SLOTS), lax.rem(i, IN_SLOTS)

    @pl.when(i == 0)
    def _():
        for j in range(IN_SLOTS):
            for c in stack_ins(j):
                c.start()
        for c in ins:
            c.start()

    for c in stack_ins(i):
        c.wait()

    @pl.when(i >= OUT_SLOTS)
    def _():
        for c in stack_outs(i - OUT_SLOTS):
            c.wait()

    @pl.when(h == 0)
    def _():
        for q in range(TWO):
            p_s[q] = times_right(e_p[g, q], block_diag(e_inv[g, q], R).T)
            rts_s[q] = scale_rows(e_rt[g, q], e_n[g, q])
        pt_s[:] = times_left(block_diag(e_inv[g, 2], R), jnp.concatenate([d_pt[g, 0], d_pt[g, 1]], 1))
        r_s[0] = d_r[g] * (1.0 - MOMENTUM)
        qpack = d_r[g] * d_n[g][:1]
        r_s[1] = qpack * step
        qrow_s[:] = qpack.T

    @pl.when(h == 1)
    def _():
        for q in range(TWO):
            p_s[q] = pltpu.roll(p_s[q], RD, 1)
            r_s[q] = pltpu.roll(r_s[q], RD, 1)

    half = pl.ds(h * RD, RD)
    for q, x in enumerate((lambda m: x_g.at[i * 2 + m], lambda m: x_u.at[ins_slot, m])):
        keep_update(p_s[q], e_rt[g, q, half], rts_s[q, half], R, x, lambda m: b_e.at[q, i * 2 + m],
                    lambda m: out_e.at[slot, q, 0, m], lambda m: out_e.at[slot, q, 1, m],
                    lambda m: outq_e.at[slot, q, m], step)
    rcopies = lane_copies(r_s[0], R, range(TWO))
    qcopies = lane_copies(r_s[1], R, range(TWO))
    pt, qrows = pt_s[half], qrow_s[half]
    for m in range(TWO):
        rows = slice(R * m, R * m + R)
        out = dot(jnp.concatenate([left_tiles(rcopies[m], R), left_tiles(qcopies[m], R)], 0), right_tiles(pt[rows], R))
        out_d[slot, 1, m] = b_d[i * 2 + m] - out[:L]
        out_d[slot, 0, m] = x_d[ins_slot, m] - out[L:]
        outq_d[slot, m] = qrows[rows]
    for c in stack_outs(i):
        c.start()

    @pl.when(i < 2 * NG - IN_SLOTS)
    def _():
        for c in stack_ins(i + IN_SLOTS):
            c.start()

    @pl.when(i == 1)
    def _():
        for c in ins:
            c.wait()
        for p0, inv, rt, n, rank, xs, b, mt, qt, size in (
                (kv_p, kv_inv, kv_rt, kv_n, R, xs_kv, b_kv, mt_kv, qt_kv, step),
                (qo_p, qo_inv, qo_rt, qo_n, RD, xs_qo, b_qo, mt_qo, qt_qo, LEARN_RATE)):
            keep_update(times_right(p0[:], block_diag(inv[:], rank).T), rt[:], scale_rows(rt[:], n[:]), rank,
                        xs.at.__getitem__, b.at.__getitem__,
                        xs.at.__getitem__, mt.at.__getitem__, qt.at.__getitem__, size)
        for c in outs:
            c.start()

    @pl.when(i == 2 * NG - 1)
    def _():
        for c in outs:
            c.wait()
        for k in range(OUT_SLOTS):
            for c in stack_outs(i - k):
                c.wait()


def run_final(xs, packs):
    hbm = pl.BlockSpec(memory_space=pl.ANY)
    v = pltpu.VMEM

    out = lambda *shape: jax.ShapeDtypeStruct(shape, F32)
    big = [out(R, H, H), out(R, H, H), out(R, R, H)]
    stacks = big + big + [out(R, L, W), out(R, L, W), out(R, R, L)]
    wide = [out(H, W), out(H, W), out(RD, W)]
    narrow = [out(H, H), out(H, H), out(R, H)]
    return pl.pallas_call(
        final_kernel,
        grid=(2 * NG,),
        out_shape=stacks + wide + narrow + narrow + wide,
        in_specs=[hbm] * len(xs) + [pl.BlockSpec(memory_space=v)] * len(packs),
        out_specs=[hbm] * len(stacks + wide + narrow + narrow + wide),
        scratch_shapes=[v((IN_SLOTS, TWO, H, H), F32), v((IN_SLOTS, TWO, L, W), F32),
                        pltpu.SemaphoreType.DMA((TWO, IN_SLOTS)), v((OUT_SLOTS, TWO, TWO, TWO, H, H), F32), v((OUT_SLOTS, TWO, TWO, R, H), F32),
                        v((OUT_SLOTS, TWO, TWO, L, W), F32), v((OUT_SLOTS, 2, R, L), F32),
                        pltpu.SemaphoreType.DMA((len(stacks), OUT_SLOTS)),
                        v((TWO, H, L), F32), v((TWO, L, H), F32), v((TWO, L, L), F32), v((L, W), F32), v((L, L), F32),
                        v((TWO, H, H), F32), v((TWO, H, W), F32), v((TWO, H, H), F32), v((TWO, H, W), F32),
                        v((TWO, R, H), F32), v((TWO, RD, W), F32),
                        pltpu.SemaphoreType.DMA((4,)), pltpu.SemaphoreType.DMA((12,))],
        name="final_kernel",
        compiler_params=pltpu.CompilerParams(vmem_limit_bytes=FINAL_VMEM, dimension_semantics=("arbitrary",)),
    )(*xs, *packs)


def solution(mesh):
    dense_w = P(('layer', 'fsdp'), 'tp')
    dense_f = P(('layer', 'tp'), None)
    stack_w = P('layer', 'fsdp', 'tp')
    stack_f = P('layer', 'tp', None)
    down_f = P('layer', 'fsdp', None)
    in_specs = (dense_w, dense_w, dense_w, dense_f) * 4 + (stack_w, stack_w, stack_w, stack_f) * 2 + (stack_w, stack_w, stack_w, down_f)
    out_specs = (dense_w, dense_w, dense_f) * 4 + (stack_w, stack_w, stack_f) * 2 + (stack_w, stack_w, down_f)

    def local_step(*b):
        x, m, g = b[0::4], b[1::4], b[2::4]
        q = [jnp.swapaxes(f, -1, -2) for f in b[3::4]]
        comm_in = []
        for i in (4, 5, 6, 0, 1, 2, 3):
            comm_in += [m[i], g[i], q[i]]
        comm_in.append(x[4])
        packs = [pltpu.with_memory_space_constraint(a, pltpu.VMEM) for a in run_comm(comm_in)]
        outs = run_final([x[i] for i in (5, 6, 0, 1, 2, 3)], packs)
        outs = list(outs[9:]) + list(outs[:9])
        for i in range(2, 21, 3):
            outs[i] = jnp.swapaxes(outs[i], -1, -2)
        return tuple(outs)

    return jax.shard_map(local_step, mesh=mesh, in_specs=in_specs, out_specs=out_specs, check_vma=False)
```
